768 devices in a mesh: rows: 48 (over y_lo, z, core), cols: 16 (over y_hi, x).
Axes of the slice: x: 4, y: 8 (y_hi: 4, y_lo: 2; y = y_hi * 2 + y_lo), z: 12, core: 2. Of those that a mesh axis runs over, the one named last changes fastest.
Arguments:
- scalar: float32 [16, 1536, 8192], P(None, 'rows', 'cols'), may hold values from -6 to 6
- diffusivity: float32 [16, 1536, 8192], P(None, 'rows', 'cols'), may hold values from 0.05 to 0.5
- vel_modes: float32 [6, 192, 1024], P(None, 'rows', 'cols'), may hold values from -8 to 8
- offsets: int32 [1536], P('rows'), may hold values from -1 to 1
Outputs:
- advanced: float32 [16, 1536, 8192], P(None, 'rows', 'cols')
The draws below stay inside these ranges and needn't reach their ends.
All inputs are finite; a program needn't handle non-finite values.
Results may differ from the reference program's by a relative error of at most 0.00007.
Values sent between devices are 32-bit elements; how exact they have to be, the bound alone decides.
No kernel may reach another device: no remote copies, remote signals or barrier semaphores. Data moves between devices by JAX's collectives and lax.ppermute only.
A program may use at most 32 MiB of HBM per device.

```python
import math
import jax
import jax.numpy as jnp
from jax import lax

PL = 16
NX = 1536
NY = 8192
NXC = 192
NYC = 1024
CZP = 3


def draw_vel_modes(key, part):
    extent = (2 * CZP, NXC, NYC)
    rough_key = jax.random.fold_in(key, 11)
    values = jax.random.truncated_normal(rough_key, -4.0, 4.0, extent, jnp.float32) * (3.5 / NYC ** 0.5)
    return jnp.clip(values, -8.0, 8.0)


def set_ends(values, own_key, least, high):
    shape = values.shape
    place = [jax.random.randint(jax.random.fold_in(own_key, axis), (), 0, shape[axis]) for axis in range(len(shape))]
    values = values.at[tuple(place)].set(least)
    longest = shape.index(max(shape))
    place[longest] = (place[longest] + 1) % shape[longest]
    return values.at[tuple(place)].set(high)


def level_of(key, shape, pieces, low, largest):
    def one(axis_at, shards_of):
        heights = jax.random.uniform(jax.random.fold_in(jax.random.fold_in(key, 6), axis_at), (shards_of,), jnp.float32, low / len(pieces), largest / len(pieces))
        return jnp.repeat(jnp.exp(heights), shape[axis_at] // shards_of).reshape((-1,) + (1,) * (len(shape) - axis_at - 1))

    gain = one(*pieces[0])
    for cut in pieces[1:]:
        gain = gain * one(*cut)
    return gain


def noise(rng, shape, width, most, cuts=(), kind=jnp.bfloat16):
    result = jax.random.normal(rng, shape, jnp.float32) * width
    if len(cuts) > 0:
        result = level_of(rng, shape, cuts, -0.22, 0.18) * result
    return jnp.clip(result, min=-most, max=most).astype(kind)


def setup_inputs(seed: int = 0) -> dict:
    key_of = jax.random.split(jax.random.key(seed), 5)
    return {
        "scalar": noise(key_of[0], (PL, NX, NY), 1.0, 6.0, ((1, 48), (2, 16)), jnp.float32),
        "diffusivity": jnp.clip(jnp.exp(math.log(0.5) - 2.3025851 * jax.random.uniform(key_of[1], (PL, NX, NY), jnp.float32) ** level_of(key_of[1], (PL, NX, NY), ((1, 48), (2, 16)), -0.2, 0.2)), 0.05, 0.5),
        "vel_modes": draw_vel_modes(jax.random.fold_in(key_of[4], 71), 0),
        "offsets": set_ends(jax.random.randint(key_of[3], (NX,), -1, 2), jax.random.fold_in(key_of[3], 1), -1, 1).astype(jnp.int32),
    }


time_step = 0.25


def window(source, row_step, col_step):
    height = source.shape[1]
    breadth = source.shape[2]
    return source[:, 2 + row_step:height - 2 + row_step, 2 + col_step:breadth - 2 + col_step]


def tendency(field, speed_rows, speed_cols, kappa):
    centre = window(field, 0, 0)
    slope_rows = (8.0 * (window(field, 1, 0) - window(field, -1, 0)) - (window(field, 2, 0) - window(field, -2, 0))) / 12.0
    slope_cols = (8.0 * (window(field, 0, 1) - window(field, 0, -1)) - (window(field, 0, 2) - window(field, 0, -2))) / 12.0
    kappa_centre = window(kappa, 0, 0)
    flux_east = 0.5 * (kappa_centre + window(kappa, 1, 0)) * (window(field, 1, 0) - centre)
    flux_west = 0.5 * (kappa_centre + window(kappa, -1, 0)) * (centre - window(field, -1, 0))
    flux_north = 0.5 * (kappa_centre + window(kappa, 0, 1)) * (window(field, 0, 1) - centre)
    flux_south = 0.5 * (kappa_centre + window(kappa, 0, -1)) * (centre - window(field, 0, -1))
    return (flux_east - flux_west) + (flux_north - flux_south) - (window(speed_rows, 0, 0) * slope_rows + window(speed_cols, 0, 0) * slope_cols)


def padded_zero(source):
    return jnp.pad(source, ((0, 0), (2, 2), (2, 2)))


def runge_kutta(field, speed_rows, speed_cols, kappa_ext, extend):
    speed_rows = padded_zero(speed_rows)
    speed_cols = padded_zero(speed_cols)
    first = tendency(extend(field), speed_rows, speed_cols, kappa_ext)
    second = tendency(extend(field + 0.5 * time_step * first), speed_rows, speed_cols, kappa_ext)
    third = tendency(extend(field + 0.5 * time_step * second), speed_rows, speed_cols, kappa_ext)
    fourth = tendency(extend(field + time_step * third), speed_rows, speed_cols, kappa_ext)
    return field + (time_step / 6.0) * (first + 2.0 * second + 2.0 * third + fourth)


def hartley_table(wavenum, places, length):
    product = (wavenum[:, None] * places[None, :]) % length
    angle = product.astype(jnp.float32) * (2.0 * jnp.pi / length)
    return jnp.cos(angle) + jnp.sin(angle)


def blend_weights(base, fraction, count):
    places = jnp.arange(count, dtype=jnp.int32)
    lower = (places[None, :] == base[:, None]).astype(jnp.float32)
    upper = (places[None, :] == ((base + 1) % count)[:, None]).astype(jnp.float32)
    return (1.0 - fraction)[:, None] * lower + fraction[:, None] * upper


def wrapped(source):
    return jnp.pad(source, ((0, 0), (2, 2), (2, 2)), mode="wrap")


def reference(scalar, diffusivity, vel_modes, offsets):
    highest = lax.Precision.HIGHEST
    coarse_planes = vel_modes.shape[0] // 2
    coarse_rows = vel_modes.shape[1]
    length = vel_modes.shape[2]
    wavenum = jnp.arange(length, dtype=jnp.int32)
    physical = jnp.einsum("cak,kb->cab", vel_modes, hartley_table(wavenum, wavenum, length), precision=highest)
    fine_rows = jnp.arange(scalar.shape[1], dtype=jnp.int32)
    row_blend = blend_weights((fine_rows // 8 + offsets) % coarse_rows, (fine_rows % 8).astype(jnp.float32) / 8.0, coarse_rows)
    fine_cols = jnp.arange(scalar.shape[2], dtype=jnp.int32)
    col_blend = blend_weights(fine_cols // 8, (fine_cols % 8).astype(jnp.float32) / 8.0, length)
    fine_planes = jnp.arange(scalar.shape[0], dtype=jnp.int32)
    plane_blend = blend_weights(fine_planes // 8, (fine_planes % 8).astype(jnp.float32) / 8.0, coarse_planes)
    along = jnp.einsum("cab,jb->caj", physical, col_blend, precision=highest)
    across = jnp.einsum("ia,caj->cij", row_blend, along, precision=highest)
    across = across.reshape(2, coarse_planes, scalar.shape[1], scalar.shape[2])

    def one_plane(items):
        field, kappa, weights = items
        speeds = jnp.einsum("q,mqij->mij", weights, across, precision=highest)
        return runge_kutta(field[None], speeds[0][None], speeds[1][None], wrapped(kappa[None]), wrapped)[0]

    return lax.map(one_plane, (scalar, diffusivity, plane_blend))
```

```python
import functools

import jax
import jax.numpy as jnp
from jax import lax
from jax.experimental import pallas as pl
from jax.experimental.pallas import tpu as pltpu
from jax.sharding import PartitionSpec as P

time_step = 0.25
HIGHEST = lax.Precision.HIGHEST

PLANES, ROWS, COLS = 16, 32, 512
GROUPS, TILES = 6, 5
HEIGHT, WIDTH = 8 * GROUPS, 128 * TILES
STRIDE = 8 * GROUPS * TILES + 8
ANY = pl.BlockSpec(memory_space=pl.ANY)
VMEM = pl.BlockSpec(memory_space=pltpu.VMEM)
EDGES = 2 * 4 * PLANES
PAYLOAD = EDGES + 4 + 3 + 1
LIMIT = 60 * 1024 * 1024


def pairing(count, shift):
    even = [(i, (i + 1) % count if (i + shift) % 2 == 0 else (i - 1) % count) for i in range(count)]
    return even


def place(rows=8, lanes=128, dim=1):
    return lax.broadcasted_iota(jnp.int32, (rows, lanes), dim)


def strip_kernel(s_ref, k_ref, first_ref, last_ref, buf, sem):
    copies = []
    for n, ref in enumerate((s_ref, k_ref)):
        for side, ct in enumerate((0, 3)):
            copy = pltpu.make_async_copy(
                ref.at[:, :, pl.ds(ct * 128, 128)], buf.at[n, side], sem.at[n, side]
            )
            copy.start()
            copies.append(copy)
    for copy in copies:
        copy.wait()
    lane = place()
    for side, out in enumerate((first_ref, last_ref)):
        for group in range(4):
            for n in range(2):
                total = jnp.zeros((8, 128), jnp.float32)
                for p in range(PLANES):
                    tile = buf[n, side, p, 8 * group : 8 * group + 8, :]
                    source = 0 if side == 0 else 120
                    moved = pltpu.roll(tile, (8 * p - source) % 128, 1)
                    total = jnp.where(lane // 8 == p, moved, total)
                out[2 * group + n] = total


def strips(scalar, diffusivity):
    return pl.pallas_call(
        strip_kernel,
        out_shape=[jax.ShapeDtypeStruct((8, 8, 128), jnp.float32)] * 2,
        in_specs=[ANY, ANY],
        out_specs=[VMEM, VMEM],
        scratch_shapes=[
            pltpu.VMEM((2, 2, PLANES, ROWS, 128), jnp.float32),
            pltpu.SemaphoreType.DMA((2, 2)),
        ],
        compiler_params=pltpu.CompilerParams(vmem_limit_bytes=8 * 1024 * 1024),
        name="strips",
    )(scalar, diffusivity)


def payload_kernel(
    s_ref, k_ref, modes_ref, cas_ref, turn_ref, before_ref, after_ref, off_ref, down_ref, up_ref, sem
):
    copies = []
    for n, ref in enumerate((s_ref, k_ref)):
        for ct in range(4):
            for side, (out, row) in enumerate(((down_ref, 0), (up_ref, ROWS - 8))):
                copy = pltpu.make_async_copy(
                    ref.at[:, pl.ds(row, 8), pl.ds(ct * 128, 128)],
                    out.at[pl.ds((4 * n + ct) * PLANES, PLANES)],
                    sem.at[n, ct, side],
                )
                copy.start()
                copies.append(copy)
    width = 128
    modes = modes_ref[...].reshape(16 * 24, 64)
    partial = jnp.dot(modes, cas_ref[...], precision=HIGHEST, preferred_element_type=jnp.float32)
    physical = jnp.zeros((24, width), jnp.float32)
    for s in range(16):
        part = partial[24 * s : 24 * s + 24]
        physical += part[:, :width] * turn_ref[s : s + 1, :] + part[:, width:] * turn_ref[16 + s : 17 + s, :]
    for out, group in ((down_ref, 0), (up_ref, 3)):
        for n in range(2):
            out[EDGES + n] = before_ref[2 * group + n]
            out[EDGES + 2 + n] = after_ref[2 * group + n]
        for i in range(3):
            out[EDGES + 4 + i] = physical[8 * i : 8 * i + 8]
        out[EDGES + 7] = jnp.broadcast_to(off_ref[...], (8, 128))
    for copy in copies:
        copy.wait()


def payloads(scalar, diffusivity, modes, cas, turn, before, after, off):
    return pl.pallas_call(
        payload_kernel,
        out_shape=[jax.ShapeDtypeStruct((PAYLOAD, 8, 128), jnp.float32)] * 2,
        in_specs=[ANY, ANY] + [VMEM] * 6,
        out_specs=[VMEM, VMEM],
        scratch_shapes=[pltpu.SemaphoreType.DMA((2, 4, 2))],
        compiler_params=pltpu.CompilerParams(vmem_limit_bytes=8 * 1024 * 1024),
        name="payloads",
    )(scalar, diffusivity, modes, cas, turn, before, after, off)


def split3(value):
    high = value.astype(jnp.bfloat16)
    rest = value - high.astype(jnp.float32)
    middle = rest.astype(jnp.bfloat16)
    low = (rest - middle.astype(jnp.float32)).astype(jnp.bfloat16)
    return high, middle, low


def shifted(value, step):
    return pltpu.roll(value, (-step) % WIDTH, 1)


def main_kernel(
    s_ref, k_ref, prev_ref, next_ref, own_ref, before_ref, after_ref, out_ref,
    raw_s, raw_k, halo, narrow, offs, own_offs, weights, state, y2, y3, y4, kt, u_ref, v_ref, cf, sem, sems,
):
    copies = []
    for n, (ref, raw) in enumerate(((s_ref, raw_s), (k_ref, raw_k))):
        for group in range(GROUPS):
            for ct in range(4):
                if group in (0, GROUPS - 1):
                    pay = prev_ref if group == 0 else next_ref
                    source = pay.at[pl.ds((4 * n + ct) * PLANES, PLANES)]
                else:
                    source = ref.at[:, pl.ds(8 * (group - 1), 8), pl.ds(128 * ct, 128)]
                copy = pltpu.make_async_copy(
                    source, raw.at[:, pl.ds((TILES * group + ct) * 8, 8), :], sem.at[n, group, ct]
                )
                copies.append(copy)
    small = [
        pltpu.make_async_copy(prev_ref.at[pl.ds(EDGES, 8)], halo.at[0], sems.at[0]),
        pltpu.make_async_copy(next_ref.at[pl.ds(EDGES, 8)], halo.at[1], sems.at[1]),
        pltpu.make_async_copy(own_ref.at[pl.ds(EDGES, 8)], halo.at[2], sems.at[2]),
        pltpu.make_async_copy(before_ref, narrow.at[0], sems.at[3]),
        pltpu.make_async_copy(after_ref, narrow.at[1], sems.at[4]),
        pltpu.make_async_copy(prev_ref.at[EDGES + 7], offs.at[0], sems.at[5]),
        pltpu.make_async_copy(next_ref.at[EDGES + 7], offs.at[1], sems.at[6]),
        pltpu.make_async_copy(own_ref.at[EDGES + 7], offs.at[2], sems.at[7]),
    ]
    for copy in small + copies:
        copy.start()
    rows_b, cols_b = (128, WIDTH)
    fine = lax.broadcasted_iota(jnp.int32, (rows_b, cols_b), 1)
    fine = jnp.where(fine < WIDTH - 64, fine, fine - WIDTH) + 8
    base = fine // 8
    part = (fine - 8 * base).astype(jnp.float32) * 0.125
    coarse = lax.broadcasted_iota(jnp.int32, (rows_b, cols_b), 0)
    blend = jnp.where(coarse == base, 1.0 - part, 0.0) + jnp.where(coarse == base + 1, part, 0.0)
    blend = blend.astype(jnp.bfloat16)
    for copy in small:
        copy.wait()
    stack = jnp.concatenate(
        [halo[j, i] for j in (0, 2, 1) for i in range(4, 7)] + [jnp.zeros((8, 128), jnp.float32)], axis=0
    )
    along = jnp.zeros((80, WIDTH), jnp.float32)
    for piece in split3(stack):
        along += jnp.dot(piece, blend, preferred_element_type=jnp.float32)
    table = jnp.concatenate(split3(along), axis=0)
    lane = place(PLANES, 256)
    local = lane % 80
    component = (local % 24) // 4
    coarse_row = ((local // 24) * 4 + local % 4 - 4).astype(jnp.float32)
    plane = lax.broadcasted_iota(jnp.int32, (PLANES, 256), 0)
    rise = (plane % 8).astype(jnp.float32) * 0.125
    scale = time_step / 24.0
    usable = jnp.logical_and(local < 72, lane < 240)
    by_plane = []
    for m in range(2):
        q = component - 3 * m
        w = jnp.where(q == plane // 8, 1.0 - rise, 0.0) + jnp.where(q == plane // 8 + 1, rise, 0.0)
        by_plane.append(jnp.where(usable, w, 0.0))
    for i in range(HEIGHT):
        if i < 8:
            shift = offs[0, 0, ROWS - 8 + i]
        elif i < 8 + ROWS:
            shift = offs[2, 0, i - 8]
        else:
            shift = offs[1, 0, i - 8 - ROWS]
        g = shift + float(i // 8 - 1)
        f = (i % 8) / 8.0
        line = jnp.where(coarse_row == g, 1.0 - f, 0.0) + jnp.where(coarse_row == g + 1.0, f, 0.0)
        for m in range(2):
            weights[m, PLANES * i : PLANES * (i + 1), :] = (by_plane[m] * line).astype(jnp.bfloat16)
    for m, speed in enumerate((u_ref, v_ref)):
        result = jnp.dot(weights[m, :, 0:240], table, preferred_element_type=jnp.float32)
        speed[...] = (result * scale).reshape(HEIGHT, PLANES, WIDTH)
    lane8 = place()
    for n, raw in enumerate((raw_s, raw_k)):
        for group in range(GROUPS):
            if group in (0, GROUPS - 1):
                j = 0 if group == 0 else 1
                left, right = halo[j, n], halo[j, 2 + n]
            else:
                left, right = narrow[0, 2 * (group - 1) + n], narrow[1, 2 * (group - 1) + n]
            for p in range(PLANES):
                a = pltpu.roll(right, (-8 * p) % 128, 1)
                b = pltpu.roll(left, (120 - 8 * p) % 128, 1)
                tile = jnp.where(lane8 < 8, a, jnp.where(lane8 >= 120, b, 0.0))
                raw[p, (TILES * group + 4) * 8 : (TILES * group + 5) * 8, :] = tile
    for copy in copies:
        copy.wait()
    flat_s = raw_s.reshape(PLANES * STRIDE, 128)
    flat_k = raw_k.reshape(PLANES * STRIDE, 128)

    @pl.loop(0, GROUPS)
    def _(group):
        for r in range(8):
            for pg in range(2):
                for ct in range(TILES):
                    start = pg * 8 * STRIDE + (TILES * group + ct) * 8 + r
                    where = (8 * group + r, slice(8 * pg, 8 * pg + 8), slice(128 * ct, 128 * ct + 128))
                    state[where] = flat_s[pl.ds(start, 8, stride=STRIDE), :]
                    kt[where] = flat_k[pl.ds(start, 8, stride=STRIDE), :] * (time_step / 4.0)

    @pl.loop(2, HEIGHT - 2)
    def _(r):
        for pg in range(2):
            at = slice(8 * pg, 8 * pg + 8)
            k = kt[r, at, :]
            ke, kw = k + kt[r + 1, at, :], k + kt[r - 1, at, :]
            kn, ks = k + shifted(k, 1), k + shifted(k, -1)
            u8, v8 = 8.0 * u_ref[r, at, :], 8.0 * v_ref[r, at, :]
            cf[0, r, at, :] = ke - u8
            cf[1, r, at, :] = kw + u8
            cf[2, r, at, :] = kn - v8
            cf[3, r, at, :] = ks + v8
            cf[4, r, at, :] = 1.0 - ((ke + kw) + (kn + ks))

    def step(y, r, at):
        c = y[r, at, :]
        total = cf[0, r, at, :] * y[r + 1, at, :] + cf[1, r, at, :] * y[r - 1, at, :]
        total += u_ref[r, at, :] * (y[r + 2, at, :] - y[r - 2, at, :])
        total += cf[2, r, at, :] * shifted(c, 1) + cf[3, r, at, :] * shifted(c, -1)
        total += v_ref[r, at, :] * (shifted(c, 2) - shifted(c, -2))
        return total + cf[4, r, at, :] * c, c

    @pl.loop(2, HEIGHT - 2)
    def _(r):
        for pg in range(2):
            at = slice(8 * pg, 8 * pg + 8)
            y2[r, at, :] = step(state, r, at)[0]

    @pl.loop(4, HEIGHT - 4)
    def _(r):
        for pg in range(2):
            at = slice(8 * pg, 8 * pg + 8)
            new, c = step(y2, r, at)
            y3[r, at, :] = state[r, at, :] + (new - c)

    @pl.loop(6, HEIGHT - 6)
    def _(r):
        for pg in range(2):
            at = slice(8 * pg, 8 * pg + 8)
            new, c = step(y3, r, at)
            y4[r, at, :] = state[r, at, :] + 2.0 * (new - c)

    third = 1.0 / 3.0

    @pl.loop(0, 4)
    def _(group):
        for q in range(8):
            r = 8 * group + 8 + q
            for pg in range(2):
                at = slice(8 * pg, 8 * pg + 8)
                new, _ = step(y4, r, at)
                total = (y2[r, at, :] + 2.0 * y3[r, at, :] - state[r, at, :] + new) * third
                for ct in range(4):
                    start = pg * 8 * STRIDE + (TILES * (group + 1) + ct) * 8 + q
                    flat_s[pl.ds(start, 8, stride=STRIDE), :] = total[:, 128 * ct : 128 * ct + 128]

    copies = []
    for group in range(4):
        for ct in range(4):
            copy = pltpu.make_async_copy(
                raw_s.at[:, pl.ds((TILES * (group + 1) + ct) * 8, 8), :],
                out_ref.at[:, pl.ds(8 * group, 8), pl.ds(128 * ct, 128)],
                sem.at[0, group, ct],
            )
            copy.start()
            copies.append(copy)
    for copy in copies:
        copy.wait()


def advance(scalar, diffusivity, prev, following, own, before, after):
    field = pltpu.VMEM((HEIGHT, PLANES, WIDTH), jnp.float32)
    return pl.pallas_call(
        main_kernel,
        out_shape=jax.ShapeDtypeStruct(scalar.shape, jnp.float32),
        in_specs=[ANY] * 7,
        out_specs=ANY,
        scratch_shapes=[
            pltpu.VMEM((PLANES, STRIDE, 128), jnp.float32),
            pltpu.VMEM((PLANES, STRIDE, 128), jnp.float32),
            pltpu.VMEM((3, 8, 8, 128), jnp.float32),
            pltpu.VMEM((2, 8, 8, 128), jnp.float32),
            pltpu.SMEM((3, 8, 128), jnp.float32),
            pltpu.SMEM((8, 128), jnp.float32),
            pltpu.VMEM((2, HEIGHT * PLANES, 256), jnp.bfloat16),
            field, field, field, field, field, field, field,
            pltpu.VMEM((5, HEIGHT, PLANES, WIDTH), jnp.float32),
            pltpu.SemaphoreType.DMA((2, GROUPS, 4)),
            pltpu.SemaphoreType.DMA((8,)),
        ],
        compiler_params=pltpu.CompilerParams(vmem_limit_bytes=LIMIT),
        name="advance",
    )(scalar, diffusivity, prev, following, own, before, after)


def angle_tables(length):
    col = lax.axis_index("cols") * 64 - 1 + jnp.arange(128, dtype=jnp.int32)
    near = jnp.arange(64, dtype=jnp.int32)[:, None] * col[None, :] % length
    far = jnp.arange(16, dtype=jnp.int32)[:, None] * 64 * col[None, :] % length
    unit = 2.0 * jnp.pi / length
    near, far = near.astype(jnp.float32) * unit, far.astype(jnp.float32) * unit
    cn, sn = jnp.cos(near), jnp.sin(near)
    cas = jnp.concatenate([cn + sn, cn - sn], axis=1)
    return cas, jnp.concatenate([jnp.cos(far), jnp.sin(far)], axis=0)


def per_device(scalar, diffusivity, vel_modes, offsets):
    length = 64 * lax.axis_size("cols")
    row_even = lax.axis_index("rows") % 2 == 0
    col_even = lax.axis_index("cols") % 2 == 0
    raw = jnp.broadcast_to(vel_modes.reshape(1, 24, 64), (16, 24, 64))
    modes = lax.all_to_all(raw, "cols", 0, 0, tiled=True)
    cas, turn = angle_tables(length)
    first, last = strips(scalar, diffusivity)
    n_cols, n_rows = lax.axis_size("cols"), lax.axis_size("rows")
    got_a = lax.ppermute(jnp.where(col_even, last, first), "cols", pairing(n_cols, 0))
    got_b = lax.ppermute(jnp.where(col_even, first, last), "cols", pairing(n_cols, 1))
    before = jnp.where(col_even, got_b, got_a)
    after = jnp.where(col_even, got_a, got_b)
    off = jnp.pad(offsets.astype(jnp.float32), (0, 96)).reshape(1, 128)
    down, up = payloads(scalar, diffusivity, modes, cas, turn, before, after, off)
    got_a = lax.ppermute(jnp.where(row_even, up, down), "rows", pairing(n_rows, 0))
    got_b = lax.ppermute(jnp.where(row_even, down, up), "rows", pairing(n_rows, 1))
    prev = jnp.where(row_even, got_b, got_a)
    following = jnp.where(row_even, got_a, got_b)
    return advance(scalar, diffusivity, prev, following, down, before, after)


def solution(mesh):
    return jax.shard_map(
        per_device,
        mesh=mesh,
        in_specs=(
            P(None, "rows", "cols"),
            P(None, "rows", "cols"),
            P(None, "rows", "cols"),
            P("rows"),
        ),
        out_specs=P(None, "rows", "cols"),
        check_vma=False,
    )
```

```python
import jax
import jax.numpy as jnp
import numpy as np
from jax import lax
from jax.experimental import pallas as pl
from jax.experimental.pallas import tpu as pltpu
from jax.sharding import PartitionSpec as P

time_step = 0.25
HIGHEST = lax.Precision.HIGHEST

PLANES, ROWS, COLS = 16, 32, 512
HEIGHT, TILES = 48, 5
WIDTH = 128 * TILES
LINE = 88
COEFS = 36
ANY = pl.BlockSpec(memory_space=pl.ANY)
VMEM = pl.BlockSpec(memory_space=pltpu.VMEM)
EDGES = 2 * 4 * PLANES
PAYLOAD = EDGES + 4 + 4 + 1
LIMIT = 60 * 1024 * 1024
BLANK = 4


def tables():
    lane = np.arange(WIDTH)
    column = 5 * (lane % 128) + lane // 128 - 8
    column = np.where(column < COLS + 8, column, -100)
    source = np.concatenate([np.arange(COLS), np.arange(128) % 8 - 8, np.arange(128) % 8 + COLS])
    spread = (source[:, None] == column[None, :]).astype(jnp.bfloat16)
    back = np.ascontiguousarray(spread[:COLS].T)
    x = np.where(column == -100, -1000, column + 8)
    base, part = x // 8, (x % 8) / 8.0
    coarse = np.arange(128)[:, None]
    blend = (coarse == base) * (1.0 - part) + (coarse == base + 1) * part
    return spread, back, blend.astype(jnp.bfloat16)


def pairing(count, shift):
    return [(i, (i + 1) % count if (i + shift) % 2 == 0 else (i - 1) % count) for i in range(count)]


def place(rows=8, lanes=128, dim=1):
    return lax.broadcasted_iota(jnp.int32, (rows, lanes), dim)


def first_kernel(s_ref, k_ref, v_ref, raw_ref, a_ref, b_ref, buf, sem):
    copies = []
    for n, ref in enumerate((s_ref, k_ref)):
        for side, ct in enumerate((0, 3)):
            copy = pltpu.make_async_copy(
                ref.at[:, :, pl.ds(ct * 128, 128)], buf.at[n, side], sem.at[n, side]
            )
            copy.start()
            copies.append(copy)
    halves = [
        jnp.concatenate([v_ref[3 * m + q] for q in range(3)] + [jnp.zeros((BLANK, 64), jnp.float32)], axis=0)
        for m in range(2)
    ]
    raw = jnp.concatenate(halves, axis=1)
    for s in range(16):
        raw_ref[s] = raw
    even = lax.rem(lax.axis_index("cols"), 2) == 0
    for copy in copies:
        copy.wait()
    lane = place()
    for group in range(4):
        for n in range(2):
            ends = []
            for side in range(2):
                total = jnp.zeros((8, 128), jnp.float32)
                for p in range(PLANES):
                    tile = buf[n, side, p, 8 * group : 8 * group + 8, :]
                    moved = pltpu.roll(tile, (8 * p - (0 if side == 0 else 120)) % 128, 1)
                    total = jnp.where(lane // 8 == p, moved, total)
                ends.append(total)
            a_ref[2 * group + n] = jnp.where(even, ends[1], ends[0])
            b_ref[2 * group + n] = jnp.where(even, ends[0], ends[1])


def first_step(scalar, diffusivity, vel_modes):
    return pl.pallas_call(
        first_kernel,
        out_shape=[jax.ShapeDtypeStruct((16, 16, 128), jnp.float32)]
        + [jax.ShapeDtypeStruct((8, 8, 128), jnp.float32)] * 2,
        in_specs=[ANY, ANY, VMEM],
        out_specs=[VMEM] * 3,
        scratch_shapes=[
            pltpu.VMEM((2, 2, PLANES, ROWS, 128), jnp.float32),
            pltpu.SemaphoreType.DMA((2, 2)),
        ],
        compiler_params=pltpu.CompilerParams(vmem_limit_bytes=LIMIT),
        name="first",
    )(scalar, diffusivity, vel_modes)


def payload_kernel(s_ref, k_ref, modes_ref, cas_ref, turn_ref, ca_ref, cb_ref, off_ref, pa_ref, pb_ref, sem):
    even = lax.rem(lax.axis_index("rows"), 2) == 0
    col_even = lax.rem(lax.axis_index("cols"), 2) == 0
    group_a = jnp.where(even, 3, 0)
    copies = []
    for side, (out, group) in enumerate(((pa_ref, group_a), (pb_ref, 3 - group_a))):
        for n, ref in enumerate((s_ref, k_ref)):
            for ct in range(4):
                copy = pltpu.make_async_copy(
                    ref.at[:, pl.ds(pl.multiple_of(8 * group, 8), 8), pl.ds(ct * 128, 128)],
                    out.at[pl.ds((4 * n + ct) * PLANES, PLANES)],
                    sem.at[n, ct, side],
                )
                copy.start()
                copies.append(copy)
    modes = modes_ref[...].reshape(16 * 16, 128)
    partial = jnp.dot(modes, cas_ref[...], precision=HIGHEST, preferred_element_type=jnp.float32)
    for m in range(2):
        physical = jnp.zeros((16, 128), jnp.float32)
        for s in range(16):
            part = partial[16 * s : 16 * s + 16, 256 * m : 256 * m + 256]
            physical += part[:, :128] * turn_ref[s : s + 1, :] + part[:, 128:] * turn_ref[16 + s : 17 + s, :]
        for out in (pa_ref, pb_ref):
            for i in range(2):
                out[EDGES + 4 + 2 * m + i] = physical[8 * i : 8 * i + 8]
    for out, group in ((pa_ref, group_a), (pb_ref, 3 - group_a)):
        for n in range(2):
            a, b = ca_ref[2 * group + n], cb_ref[2 * group + n]
            out[EDGES + n] = jnp.where(col_even, b, a)
            out[EDGES + 2 + n] = jnp.where(col_even, a, b)
        out[EDGES + 8] = jnp.broadcast_to(off_ref[...], (8, 128))
    for copy in copies:
        copy.wait()


def payloads(*args):
    return pl.pallas_call(
        payload_kernel,
        out_shape=[jax.ShapeDtypeStruct((PAYLOAD, 8, 128), jnp.float32)] * 2,
        in_specs=[ANY, ANY] + [VMEM] * 6,
        out_specs=[VMEM, VMEM],
        scratch_shapes=[pltpu.SemaphoreType.DMA((2, 4, 2))],
        compiler_params=pltpu.CompilerParams(vmem_limit_bytes=LIMIT),
        name="payloads",
    )(*args)


def split2(value):
    high = value.astype(jnp.bfloat16)
    return high, (value - high.astype(jnp.float32)).astype(jnp.bfloat16)


def split3(value):
    high, _ = split2(value)
    middle, low = split2(value - high.astype(jnp.float32))
    return high, middle, low


def spread_lhs(lhs, row, tiles):
    for c, tile in enumerate(tiles):
        high, low = split2(tile)
        lhs[pl.ds(row, 16), 128 * c : 128 * c + 128] = high
        lhs[pl.ds(row, 16), 768 + 128 * c : 896 + 128 * c] = low


def doubled(ref, table, sem):
    rows = ref.shape[0]
    return [pltpu.make_async_copy(ref, table.at[pl.ds(half * rows, rows), :], sem.at[half]) for half in range(2)]


def own_kernel(s_ref, k_ref, ca_ref, cb_ref, spread_ref, out_ref, raw, strip, lhs, spread, res, inner, sem, sems, out_sem):
    col_even = lax.rem(lax.axis_index("cols"), 2) == 0
    big = [pltpu.make_async_copy(ref, raw.at[n], sem.at[n]) for n, ref in enumerate((k_ref, s_ref))]
    late = doubled(spread_ref, spread, sems)
    for copy in big + late:
        copy.start()
    for n in range(2):
        for group in range(4):
            a, b = ca_ref[2 * group + 1 - n], cb_ref[2 * group + 1 - n]
            strip[n, 0, 8 * group : 8 * group + 8, :] = jnp.where(col_even, b, a)
            strip[n, 1, 8 * group : 8 * group + 8, :] = jnp.where(col_even, a, b)
    owner = place(16, 128) // 8
    for copy in big + late:
        copy.wait()

    @pl.loop(0, 2)
    def _(n):
        scale = jnp.where(n == 0, time_step / 4.0, 1.0)

        @pl.loop(0, PLANES)
        def _(p):
            for g in range(2):
                at = slice(16 * g, 16 * g + 16)
                tiles = [raw[n, p, at, 128 * c : 128 * c + 128] for c in range(4)]
                tiles += [jnp.where(owner == p, strip[n, side, at, :], 0.0) for side in range(2)]
                spread_lhs(lhs, pl.multiple_of(ROWS * p + 16 * g, 16), tiles)

        res[...] = jnp.dot(lhs[...], spread[...], preferred_element_type=jnp.float32)

        @pl.loop(0, ROWS // 8)
        def _(g):
            for p in range(PLANES):
                for t in range(TILES):
                    tile = res[pl.ds(pl.multiple_of(ROWS * p + 8 * g, 8), 8), 128 * t : 128 * t + 128] * scale
                    start = 8 * g * LINE + 40 * (p // 8) + 8 * t + p % 8
                    inner[n, pl.ds(start, 8, stride=LINE), :] = tile

        pltpu.make_async_copy(inner.at[n], out_ref.at[n], out_sem.at[n]).start()

    for n in range(2):
        pltpu.make_async_copy(inner.at[n], out_ref.at[n], out_sem.at[n]).wait()


def own_rows(scalar, diffusivity, ca, cb, spread):
    return pl.pallas_call(
        own_kernel,
        out_shape=jax.ShapeDtypeStruct((2, ROWS * LINE, 128), jnp.float32),
        in_specs=[ANY, ANY, VMEM, VMEM, ANY],
        out_specs=ANY,
        scratch_shapes=[
            pltpu.VMEM((2, PLANES, ROWS, COLS), jnp.float32),
            pltpu.VMEM((2, 2, ROWS, 128), jnp.float32),
            pltpu.VMEM((ROWS * PLANES, 1536), jnp.bfloat16),
            pltpu.VMEM((1536, WIDTH), jnp.bfloat16),
            pltpu.VMEM((ROWS * PLANES, WIDTH), jnp.float32),
            pltpu.VMEM((2, ROWS * LINE, 128), jnp.float32),
            pltpu.SemaphoreType.DMA((2,)),
            pltpu.SemaphoreType.DMA((2,)),
            pltpu.SemaphoreType.DMA((2,)),
        ],
        compiler_params=pltpu.CompilerParams(vmem_limit_bytes=LIMIT),
        cost_estimate=pl.CostEstimate(flops=2_000_000_000, bytes_accessed=8_000_000, transcendentals=0),
        name="own_rows",
    )(scalar, diffusivity, ca, cb, spread)


def main_kernel(
    own_ref, ra_ref, rb_ref, pay_ref, spread_ref, back_ref, blend_ref, out_ref,
    raw, halo, offs, weights, lhs, spread, back, blend, res,
    field, y2, y3, y4, cf, final, result, sem, sems, out_sem,
):
    even = lax.rem(lax.axis_index("rows"), 2) == 0
    slot_a = jnp.where(even, 1, 0)
    kt, state = field.at[0], field.at[1]
    edges = []
    for side, (pay, slot) in enumerate(((ra_ref, slot_a), (rb_ref, 1 - slot_a))):
        for n in range(2):
            for ct in range(4):
                edges.append(
                    pltpu.make_async_copy(
                        pay.at[pl.ds((4 * (1 - n) + ct) * PLANES, PLANES)],
                        raw.at[n, :, pl.ds(pl.multiple_of(8 * slot, 8), 8), pl.ds(128 * ct, 128)],
                        sem.at[side, n, ct],
                    )
                )
    small = [
        pltpu.make_async_copy(ra_ref.at[pl.ds(EDGES, 8)], halo.at[slot_a], sems.at[0]),
        pltpu.make_async_copy(rb_ref.at[pl.ds(EDGES, 8)], halo.at[1 - slot_a], sems.at[1]),
        pltpu.make_async_copy(pay_ref.at[pl.ds(EDGES, 8)], halo.at[2], sems.at[2]),
        pltpu.make_async_copy(ra_ref.at[EDGES + 8], offs.at[slot_a], sems.at[3]),
        pltpu.make_async_copy(rb_ref.at[EDGES + 8], offs.at[1 - slot_a], sems.at[4]),
        pltpu.make_async_copy(pay_ref.at[EDGES + 8], offs.at[2], sems.at[5]),
        pltpu.make_async_copy(blend_ref, blend, sems.at[6]),
    ]
    late = doubled(spread_ref, spread, sems.at[pl.ds(7, 2)])
    last = doubled(back_ref, back, sems.at[pl.ds(9, 2)])
    own = [
        pltpu.make_async_copy(own_ref.at[n], field.at[n, pl.ds(8 * LINE, ROWS * LINE), :], sems.at[11 + n])
        for n in range(2)
    ]
    for copy in small + edges + late + own + last:
        copy.start()
    lane = place(PLANES, 256)
    local = lane % 48
    plane = lax.broadcasted_iota(jnp.int32, (PLANES, 256), 0)
    rise = (plane % 8).astype(jnp.float32) * 0.125
    q = (local % 16) // 4
    by_plane = jnp.where(q == plane // 8, 1.0 - rise, 0.0) + jnp.where(q == plane // 8 + 1, rise, 0.0)
    by_plane = jnp.where(jnp.logical_and(q < 3, lane < 144), by_plane, 0.0)
    coarse_row = ((local // 16) * 4 + local % 4 - 4).astype(jnp.float32)
    for copy in small:
        copy.wait()

    @pl.loop(0, HEIGHT // 8)
    def _(group):
        block = jnp.where(group == 0, 0, jnp.where(group == 5, 1, 2))
        start = jnp.where(group == 0, ROWS - 8, jnp.where(group == 5, 0, 8 * (group - 1)))
        for i in range(8):
            g = offs[block, 0, start + i] + (group - 1).astype(jnp.float32)
            f = i / 8.0
            line = jnp.where(coarse_row == g, 1.0 - f, 0.0) + jnp.where(coarse_row == g + 1.0, f, 0.0)
            row = pl.multiple_of(PLANES * (8 * group + i), 16)
            weights[pl.ds(row, PLANES), :] = (by_plane * line).astype(jnp.bfloat16)

    @pl.loop(0, 2)
    def _(m):
        stack = jnp.concatenate([halo[j, 4 + 2 * m + i] for j in (0, 2, 1) for i in range(2)], axis=0)
        pieces = jnp.concatenate(split3(stack), axis=0)
        parts = jnp.dot(pieces, blend[...], preferred_element_type=jnp.float32)
        along = (parts[0:48] + parts[48:96] + parts[96:144]) * (time_step / 24.0)
        table = jnp.concatenate(split3(along), axis=0)
        res[...] = jnp.dot(weights[:, 0:144], table, preferred_element_type=jnp.float32)

        @pl.loop(0, HEIGHT // 2)
        def _(i):
            for j in range(4):
                for t in range(TILES):
                    row = pl.multiple_of((i * 4 + j) * (8 * COEFS) + 8 * (5 * (5 + m) + t), 8)
                    cf[pl.ds(row, 8), :] = res[
                        pl.ds(pl.multiple_of(32 * i + 8 * j, 8), 8), 128 * t : 128 * t + 128
                    ]

    owner = place(16, 128) // 8
    for copy in edges + late:
        copy.wait()

    @pl.loop(0, 2)
    def _(n):
        @pl.loop(0, PLANES)
        def _(p):
            tiles = [raw[n, p, :, 128 * c : 128 * c + 128] for c in range(4)]
            for side in range(2):
                both = jnp.concatenate([halo[j, 2 * side + 1 - n] for j in range(2)], axis=0)
                tiles.append(jnp.where(owner == p, both, 0.0))
            spread_lhs(lhs, pl.multiple_of(256 * n + 16 * p, 16), tiles)

    res[0:512, :] = jnp.dot(lhs[...], spread[...], preferred_element_type=jnp.float32)

    @pl.loop(0, 2)
    def _(n):
        scale = jnp.where(n == 0, time_step / 4.0, 1.0)
        for j in range(2):
            for p in range(PLANES):
                for t in range(TILES):
                    row = pl.multiple_of(256 * n + 16 * p + 8 * j, 8)
                    tile = res[pl.ds(row, 8), 128 * t : 128 * t + 128] * scale
                    start = 40 * j * LINE + 40 * (p // 8) + 8 * t + p % 8
                    field[n, pl.ds(start, 8, stride=LINE), :] = tile

    for copy in own:
        copy.wait()

    def tile(ref, r, pg, t):
        return ref[pl.ds(pl.multiple_of(r * LINE + 40 * pg + 8 * t, 8), 8), :]

    def put(ref, r, pg, t, value):
        ref[pl.ds(pl.multiple_of(r * LINE + 40 * pg + 8 * t, 8), 8), :] = value

    def coef(r, pg, c, t):
        return pl.ds(pl.multiple_of((r * 2 + pg) * (8 * COEFS) + 8 * (5 * c + t), 8), 8)

    def rows(low, high):
        def wrap(body):
            @pl.loop(0, (high - low) // 4)
            def _(i):
                for j in range(4):
                    body(low + 4 * i + j)

        return wrap

    @rows(2, HEIGHT - 2)
    def _(r):
        for pg in range(2):
            k = [tile(kt, r, pg, t) for t in range(TILES)]
            nxt = k[1:] + [pltpu.roll(k[0], 127, 1)]
            prv = [pltpu.roll(k[4], 1, 1)] + k[:4]
            for t in range(TILES):
                ke, kw = k[t] + tile(kt, r + 1, pg, t), k[t] + tile(kt, r - 1, pg, t)
                kn, ks = k[t] + nxt[t], k[t] + prv[t]
                u8, v8 = 8.0 * cf[coef(r, pg, 5, t), :], 8.0 * cf[coef(r, pg, 6, t), :]
                cf[coef(r, pg, 0, t), :] = ke - u8
                cf[coef(r, pg, 1, t), :] = kw + u8
                cf[coef(r, pg, 2, t), :] = kn - v8
                cf[coef(r, pg, 3, t), :] = ks + v8
                cf[coef(r, pg, 4, t), :] = 1.0 - ((ke + kw) + (kn + ks))

    def step(y, r, pg):
        c = [tile(y, r, pg, t) for t in range(TILES)]
        first, second = pltpu.roll(c[0], 127, 1), pltpu.roll(c[1], 127, 1)
        last, before = pltpu.roll(c[4], 1, 1), pltpu.roll(c[3], 1, 1)
        ext = [before, last] + c + [first, second]
        new = []
        for t in range(TILES):
            total = cf[coef(r, pg, 0, t), :] * tile(y, r + 1, pg, t) + cf[coef(r, pg, 1, t), :] * tile(y, r - 1, pg, t)
            total += cf[coef(r, pg, 5, t), :] * (tile(y, r + 2, pg, t) - tile(y, r - 2, pg, t))
            along = cf[coef(r, pg, 2, t), :] * ext[t + 3] + cf[coef(r, pg, 3, t), :] * ext[t + 1]
            along += cf[coef(r, pg, 6, t), :] * (ext[t + 4] - ext[t])
            new.append(total + along + cf[coef(r, pg, 4, t), :] * c[t])
        return new, c

    @rows(2, HEIGHT - 2)
    def _(r):
        for pg in range(2):
            new, _ = step(state, r, pg)
            for t in range(TILES):
                put(y2, r, pg, t, new[t])

    @rows(4, HEIGHT - 4)
    def _(r):
        for pg in range(2):
            new, c = step(y2, r, pg)
            for t in range(TILES):
                put(y3, r, pg, t, tile(state, r, pg, t) + (new[t] - c[t]))

    @rows(6, HEIGHT - 6)
    def _(r):
        for pg in range(2):
            new, c = step(y3, r, pg)
            for t in range(TILES):
                put(y4, r, pg, t, tile(state, r, pg, t) + 2.0 * (new[t] - c[t]))

    third = 1.0 / 3.0

    @rows(0, ROWS)
    def _(q):
        r = q + 8
        for pg in range(2):
            new, _ = step(y4, r, pg)
            for t in range(TILES):
                total = (tile(y2, r, pg, t) - tile(state, r, pg, t)) + (2.0 * tile(y3, r, pg, t) + new[t])
                start = 168 * 8 * pg + 8 * (5 * (q // 8) + t) + q % 8
                final[pl.ds(start, 8, stride=168), :] = total * third

    @pl.loop(0, PLANES)
    def _(p):
        for g in range(2):
            rows = pl.ds(pl.multiple_of(32 * p + 16 * g, 16), 16)
            for t in range(TILES):
                both = [
                    final[pl.ds(pl.multiple_of(168 * p + 8 * (5 * (2 * g + i) + t), 8), 8), :] for i in range(2)
                ]
                high, low = split2(jnp.concatenate(both, axis=0))
                lhs[rows, 128 * t : 128 * t + 128] = high
                lhs[rows, WIDTH + 128 * t : WIDTH + 128 * t + 128] = low

    for copy in last:
        copy.wait()
    copies = []
    for half in range(2):
        rows = 8 * ROWS
        result[8 * half : 8 * half + 8] = jnp.dot(
            lhs[rows * half : rows * (half + 1), 0 : 2 * WIDTH], back[...], preferred_element_type=jnp.float32
        ).reshape(8, ROWS, COLS)
        copy = pltpu.make_async_copy(
            result.at[pl.ds(8 * half, 8)], out_ref.at[pl.ds(8 * half, 8)], out_sem.at[half]
        )
        copy.start()
        copies.append(copy)
    for copy in copies:
        copy.wait()


def advance(shape, own, ra, rb, pay, spread, back, blend):
    line = pltpu.VMEM((HEIGHT * LINE, 128), jnp.float32)
    return pl.pallas_call(
        main_kernel,
        out_shape=jax.ShapeDtypeStruct(shape, jnp.float32),
        in_specs=[ANY] * 7,
        out_specs=ANY,
        scratch_shapes=[
            pltpu.VMEM((2, PLANES, 16, COLS), jnp.float32),
            pltpu.VMEM((3, 8, 8, 128), jnp.float32),
            pltpu.SMEM((3, 8, 128), jnp.float32),
            pltpu.VMEM((HEIGHT * PLANES, 256), jnp.bfloat16),
            pltpu.VMEM((ROWS * PLANES, 1536), jnp.bfloat16),
            pltpu.VMEM((1536, WIDTH), jnp.bfloat16),
            pltpu.VMEM((2 * WIDTH, COLS), jnp.bfloat16),
            pltpu.VMEM((128, WIDTH), jnp.bfloat16),
            pltpu.VMEM((HEIGHT * PLANES, WIDTH), jnp.float32),
            pltpu.VMEM((2, HEIGHT * LINE, 128), jnp.float32),
            line, line, line,
            pltpu.VMEM((HEIGHT * 2 * COEFS * 8, 128), jnp.float32),
            pltpu.VMEM((PLANES * 168, 128), jnp.float32),
            pltpu.VMEM((PLANES, ROWS, COLS), jnp.float32),
            pltpu.SemaphoreType.DMA((2, 2, 4)),
            pltpu.SemaphoreType.DMA((13,)),
            pltpu.SemaphoreType.DMA((2,)),
        ],
        compiler_params=pltpu.CompilerParams(vmem_limit_bytes=LIMIT),
        name="advance",
    )(own, ra, rb, pay, spread, back, blend)


def angle_tables(length):
    col = lax.axis_index("cols") * 64 - 1 + jnp.arange(128, dtype=jnp.int32)
    near = jnp.arange(64, dtype=jnp.int32)[:, None] * col[None, :] % length
    far = jnp.arange(16, dtype=jnp.int32)[:, None] * 64 * col[None, :] % length
    unit = 2.0 * jnp.pi / length
    near, far = near.astype(jnp.float32) * unit, far.astype(jnp.float32) * unit
    cn, sn = jnp.cos(near), jnp.sin(near)
    cas, zero = jnp.concatenate([cn + sn, cn - sn], axis=1), jnp.zeros((64, 256), jnp.float32)
    cas = jnp.concatenate([jnp.concatenate([cas, zero], axis=1), jnp.concatenate([zero, cas], axis=1)], axis=0)
    return cas, jnp.concatenate([jnp.cos(far), jnp.sin(far)], axis=0)


def per_device(scalar, diffusivity, vel_modes, offsets):
    n_cols, n_rows = lax.axis_size("cols"), lax.axis_size("rows")
    raw, a, b = first_step(scalar, diffusivity, vel_modes)
    modes = lax.all_to_all(raw, "cols", 0, 0, tiled=True)
    cas, turn = angle_tables(64 * n_cols)
    ca = lax.ppermute(a, "cols", pairing(n_cols, 0))
    cb = lax.ppermute(b, "cols", pairing(n_cols, 1))
    off = jnp.pad(offsets.astype(jnp.float32), (0, 96)).reshape(1, 128)
    pa, pb = payloads(scalar, diffusivity, modes, cas, turn, ca, cb, off)
    ra = lax.ppermute(pa, "rows", pairing(n_rows, 0))
    rb = lax.ppermute(pb, "rows", pairing(n_rows, 1))
    spread, back, blend = (jnp.asarray(table) for table in tables())
    ca, cb, _ = lax.optimization_barrier((ca, cb, pa))
    own = own_rows(scalar, diffusivity, ca, cb, spread)
    return advance(scalar.shape, own, ra, rb, pa, spread, back, blend)


def solution(mesh):
    return jax.shard_map(
        per_device,
        mesh=mesh,
        in_specs=(
            P(None, "rows", "cols"),
            P(None, "rows", "cols"),
            P(None, "rows", "cols"),
            P("rows"),
        ),
        out_specs=P(None, "rows", "cols"),
        check_vma=False,
    )
```

```python
import jax
import jax.numpy as jnp
import numpy as np
from jax import lax
from jax.experimental import pallas as pl
from jax.experimental.pallas import tpu as pltpu
from jax.sharding import PartitionSpec as P

time_step = 0.25
HIGHEST = lax.Precision.HIGHEST

PLANES, ROWS, COLS = 16, 32, 512
HEIGHT, TILES = 48, 5
WIDTH = 128 * TILES
LINE = 88
COEFS = 36
ANY = pl.BlockSpec(memory_space=pl.ANY)
HBM = pl.BlockSpec(memory_space=pltpu.HBM)
VMEM = pl.BlockSpec(memory_space=pltpu.VMEM)
EDGES = 2 * 4 * PLANES
PAYLOAD = EDGES + 4 + 4 + 1
LIMIT = 67043328
BLANK = 4


def tables():
    lane = np.arange(WIDTH)
    column = 5 * (lane % 128) + lane // 128 - 8
    column = np.where(column < COLS + 8, column, -100)
    source = np.concatenate([np.arange(COLS), np.arange(128) % 8 - 8, np.arange(128) % 8 + COLS])
    spread = (source[:, None] == column[None, :]).astype(jnp.bfloat16)
    back = np.ascontiguousarray(spread[:COLS].T)
    x = np.where(column == -100, -1000, column + 8)
    base, part = x // 8, (x % 8) / 8.0
    coarse = np.arange(128)[:, None]
    blend = (coarse == base) * (1.0 - part) + (coarse == base + 1) * part
    return spread, back, blend.astype(jnp.bfloat16)


def pairing(count, shift):
    return [(i, (i + 1) % count if (i + shift) % 2 == 0 else (i - 1) % count) for i in range(count)]


def place(rows=8, lanes=128, dim=1):
    return lax.broadcasted_iota(jnp.int32, (rows, lanes), dim)


def first_kernel(s_ref, k_ref, v_hbm, raw_ref, a_ref, b_ref, buf, v_ref, sem, v_sem):
    modes = pltpu.make_async_copy(v_hbm, v_ref, v_sem)
    modes.start()
    copies = []
    for n, ref in enumerate((s_ref, k_ref)):
        for side, ct in enumerate((0, 3)):
            copy = pltpu.make_async_copy(
                ref.at[:, :, pl.ds(ct * 128, 128)], buf.at[n, side], sem.at[n, side]
            )
            copy.start()
            copies.append(copy)
    modes.wait()
    halves = [
        jnp.concatenate([v_ref[3 * m + q] for q in range(3)] + [jnp.zeros((BLANK, 64), jnp.float32)], axis=0)
        for m in range(2)
    ]
    raw = jnp.concatenate(halves, axis=1)
    for s in range(16):
        raw_ref[s] = raw
    even = lax.rem(lax.axis_index("cols"), 2) == 0
    for copy in copies:
        copy.wait()
    lane = place()
    for group in range(4):
        for n in range(2):
            ends = []
            for side in range(2):
                total = jnp.zeros((8, 128), jnp.float32)
                for p in range(PLANES):
                    tile = buf[n, side, p, 8 * group : 8 * group + 8, :]
                    moved = pltpu.roll(tile, (8 * p - (0 if side == 0 else 120)) % 128, 1)
                    total = jnp.where(lane // 8 == p, moved, total)
                ends.append(total)
            a_ref[2 * group + n] = jnp.where(even, ends[1], ends[0])
            b_ref[2 * group + n] = jnp.where(even, ends[0], ends[1])


def first_step(scalar, diffusivity, vel_modes):
    return pl.pallas_call(
        first_kernel,
        out_shape=[jax.ShapeDtypeStruct((16, 16, 128), jnp.float32)]
        + [jax.ShapeDtypeStruct((8, 8, 128), jnp.float32)] * 2,
        in_specs=[HBM, HBM, HBM],
        out_specs=[VMEM] * 3,
        scratch_shapes=[
            pltpu.VMEM((2, 2, PLANES, ROWS, 128), jnp.float32),
            pltpu.VMEM((6, 4, 64), jnp.float32),
            pltpu.SemaphoreType.DMA((2, 2)),
            pltpu.SemaphoreType.DMA,
        ],
        compiler_params=pltpu.CompilerParams(vmem_limit_bytes=LIMIT),
        name="first",
    )(scalar, diffusivity, vel_modes)


def payload_kernel(
    s_ref, k_ref, modes_hbm, cas_ref, turn_hbm, ca_hbm, cb_hbm, off_hbm, pa_ref, pb_ref,
    stage, cas, modes_ref, turn_ref, ca_ref, cb_ref, off_ref, sem, cas_sem, out_sem,
):
    even = lax.rem(lax.axis_index("rows"), 2) == 0
    column = lax.axis_index("cols")
    fetch = [
        pltpu.make_async_copy(
            cas_ref.at[column], cas.at[pl.ds(64 * m, 64), pl.ds(256 * m, 256)], cas_sem.at[m]
        )
        for m in range(2)
    ]
    for i, (source, target) in enumerate(
        ((modes_hbm, modes_ref), (turn_hbm, turn_ref), (ca_hbm, ca_ref), (cb_hbm, cb_ref), (off_hbm, off_ref))
    ):
        fetch.append(pltpu.make_async_copy(source, target, cas_sem.at[2 + i]))
    for copy in fetch:
        copy.start()
    for m in range(2):
        cas[64 * m : 64 * m + 64, 256 * (1 - m) : 256 * (2 - m)] = jnp.zeros((64, 256), jnp.float32)
    col_even = lax.rem(lax.axis_index("cols"), 2) == 0
    group_a = jnp.where(even, 3, 0)
    copies = []
    for side, group in enumerate((group_a, 3 - group_a)):
        for n, ref in enumerate((s_ref, k_ref)):
            for ct in range(4):
                copy = pltpu.make_async_copy(
                    ref.at[:, pl.ds(pl.multiple_of(8 * group, 8), 8), pl.ds(ct * 128, 128)],
                    stage.at[side, pl.ds((4 * n + ct) * PLANES, PLANES)],
                    sem.at[n, ct, side],
                )
                copy.start()
                copies.append(copy)
    for copy in fetch:
        copy.wait()
    modes = modes_ref[...].reshape(16 * 16, 128)
    sent = []
    for side, out in enumerate((pa_ref, pb_ref)):
        for copy in copies[8 * side : 8 * side + 8]:
            copy.wait()
        copy = pltpu.make_async_copy(
            stage.at[side, pl.ds(0, EDGES)], out.at[pl.ds(0, EDGES)], out_sem.at[side, 0]
        )
        copy.start()
        sent.append(copy)
    partial = jnp.dot(modes, cas[...], precision=HIGHEST, preferred_element_type=jnp.float32)
    for m in range(2):
        physical = jnp.zeros((16, 128), jnp.float32)
        for s in range(16):
            part = partial[16 * s : 16 * s + 16, 256 * m : 256 * m + 256]
            physical += part[:, :128] * turn_ref[s : s + 1, :] + part[:, 128:] * turn_ref[16 + s : 17 + s, :]
        for side in range(2):
            for i in range(2):
                stage[side, EDGES + 4 + 2 * m + i] = physical[8 * i : 8 * i + 8]
    for side, (out, group) in enumerate(((pa_ref, group_a), (pb_ref, 3 - group_a))):
        for n in range(2):
            a, b = ca_ref[2 * group + n], cb_ref[2 * group + n]
            stage[side, EDGES + n] = jnp.where(col_even, b, a)
            stage[side, EDGES + 2 + n] = jnp.where(col_even, a, b)
        line = jnp.concatenate([off_ref[...].astype(jnp.float32), jnp.zeros((1, 96), jnp.float32)], axis=1)
        stage[side, EDGES + 8] = jnp.broadcast_to(line, (8, 128))
        copy = pltpu.make_async_copy(
            stage.at[side, pl.ds(EDGES, 9)], out.at[pl.ds(EDGES, 9)], out_sem.at[side, 1]
        )
        copy.start()
        sent.append(copy)
    for copy in sent:
        copy.wait()


def payloads(*args):
    return pl.pallas_call(
        payload_kernel,
        out_shape=[jax.ShapeDtypeStruct((PAYLOAD, 8, 128), jnp.float32)] * 2,
        in_specs=[HBM] * 8,
        out_specs=[HBM, HBM],
        scratch_shapes=[
            pltpu.VMEM((2, PAYLOAD, 8, 128), jnp.float32),
            pltpu.VMEM((128, 512), jnp.float32),
            pltpu.VMEM((16, 16, 128), jnp.float32),
            pltpu.VMEM((32, 128), jnp.float32),
            pltpu.VMEM((8, 8, 128), jnp.float32),
            pltpu.VMEM((8, 8, 128), jnp.float32),
            pltpu.VMEM((1, 32), jnp.int32),
            pltpu.SemaphoreType.DMA((2, 4, 2)),
            pltpu.SemaphoreType.DMA((7,)),
            pltpu.SemaphoreType.DMA((2, 2)),
        ],
        compiler_params=pltpu.CompilerParams(vmem_limit_bytes=LIMIT),
        name="payloads",
    )(*args)


def split2(value):
    high = value.astype(jnp.bfloat16)
    return high, (value - high.astype(jnp.float32)).astype(jnp.bfloat16)


def split3(value):
    high, _ = split2(value)
    middle, low = split2(value - high.astype(jnp.float32))
    return high, middle, low


def spread_lhs(lhs, row, tiles):
    for c, tile in enumerate(tiles):
        high, low = split2(tile)
        lhs[pl.ds(row, 16), 128 * c : 128 * c + 128] = high
        lhs[pl.ds(row, 16), 768 + 128 * c : 896 + 128 * c] = low


def doubled(ref, table, sem):
    rows = ref.shape[0]
    return [pltpu.make_async_copy(ref, table.at[pl.ds(half * rows, rows), :], sem.at[half]) for half in range(2)]


def own_kernel(
    s_ref, k_ref, ca_hbm, cb_hbm, spread_ref, out_ref,
    raw, cols, strip, lhs, spread, res, inner, sem, sems, out_sem,
):
    col_even = lax.rem(lax.axis_index("cols"), 2) == 0
    big = [pltpu.make_async_copy(ref, raw.at[n], sem.at[n]) for n, ref in enumerate((k_ref, s_ref))]
    late = doubled(spread_ref, spread, sems)
    small = [
        pltpu.make_async_copy(ref, cols.at[side], sems.at[2 + side]) for side, ref in enumerate((ca_hbm, cb_hbm))
    ]
    for copy in small + big[:1] + late + big[1:]:
        copy.start()
    for copy in small:
        copy.wait()
    for n in range(2):
        for group in range(4):
            a, b = cols[0, 2 * group + 1 - n], cols[1, 2 * group + 1 - n]
            strip[n, 0, 8 * group : 8 * group + 8, :] = jnp.where(col_even, b, a)
            strip[n, 1, 8 * group : 8 * group + 8, :] = jnp.where(col_even, a, b)
    owner = place(16, 128) // 8
    for copy in big + late:
        copy.wait()

    @pl.loop(0, 2)
    def _(n):
        scale = jnp.where(n == 0, time_step / 4.0, 1.0)

        @pl.loop(0, PLANES)
        def _(p):
            for g in range(2):
                at = slice(16 * g, 16 * g + 16)
                tiles = [raw[n, p, at, 128 * c : 128 * c + 128] for c in range(4)]
                tiles += [jnp.where(owner == p, strip[n, side, at, :], 0.0) for side in range(2)]
                spread_lhs(lhs, pl.multiple_of(ROWS * p + 16 * g, 16), tiles)

        res[...] = jnp.dot(lhs[...], spread[...], preferred_element_type=jnp.float32)

        @pl.loop(0, ROWS // 8)
        def _(g):
            for p in range(PLANES):
                for t in range(TILES):
                    tile = res[pl.ds(pl.multiple_of(ROWS * p + 8 * g, 8), 8), 128 * t : 128 * t + 128] * scale
                    start = 8 * g * LINE + 40 * (p // 8) + 8 * t + p % 8
                    inner[n, pl.ds(start, 8, stride=LINE), :] = tile

        pltpu.make_async_copy(inner.at[n], out_ref.at[n], out_sem.at[n]).start()

    for n in range(2):
        pltpu.make_async_copy(inner.at[n], out_ref.at[n], out_sem.at[n]).wait()


def own_rows(scalar, diffusivity, ca, cb, spread):
    return pl.pallas_call(
        own_kernel,
        out_shape=jax.ShapeDtypeStruct((2, ROWS * LINE, 128), jnp.float32),
        in_specs=[HBM] * 5,
        out_specs=HBM,
        scratch_shapes=[
            pltpu.VMEM((2, PLANES, ROWS, COLS), jnp.float32),
            pltpu.VMEM((2, 8, 8, 128), jnp.float32),
            pltpu.VMEM((2, 2, ROWS, 128), jnp.float32),
            pltpu.VMEM((ROWS * PLANES, 1536), jnp.bfloat16),
            pltpu.VMEM((1536, WIDTH), jnp.bfloat16),
            pltpu.VMEM((ROWS * PLANES, WIDTH), jnp.float32),
            pltpu.VMEM((2, ROWS * LINE, 128), jnp.float32),
            pltpu.SemaphoreType.DMA((2,)),
            pltpu.SemaphoreType.DMA((4,)),
            pltpu.SemaphoreType.DMA((2,)),
        ],
        compiler_params=pltpu.CompilerParams(vmem_limit_bytes=LIMIT),
        cost_estimate=pl.CostEstimate(flops=2_000_000_000, bytes_accessed=8_000_000, transcendentals=0),
        name="own_rows",
    )(scalar, diffusivity, ca, cb, spread)


def main_kernel(
    own_ref, ra_ref, rb_ref, pay_ref, spread_ref, back_ref, blend_ref, out_ref,
    raw, halo, offs, weights, lhs, spread, back, blend, res,
    field, y2, y3, y4, cf, final, result, sem, sems, out_sem,
):
    even = lax.rem(lax.axis_index("rows"), 2) == 0
    slot_a = jnp.where(even, 1, 0)
    kt, state = field.at[0], field.at[1]
    edges = []
    for side, (pay, slot) in enumerate(((ra_ref, slot_a), (rb_ref, 1 - slot_a))):
        for n in range(2):
            for ct in range(4):
                edges.append(
                    pltpu.make_async_copy(
                        pay.at[pl.ds((4 * (1 - n) + ct) * PLANES, PLANES)],
                        raw.at[n, :, pl.ds(pl.multiple_of(8 * slot, 8), 8), pl.ds(128 * ct, 128)],
                        sem.at[side, n, ct],
                    )
                )
    small = [
        pltpu.make_async_copy(ra_ref.at[pl.ds(EDGES, 8)], halo.at[slot_a], sems.at[0]),
        pltpu.make_async_copy(rb_ref.at[pl.ds(EDGES, 8)], halo.at[1 - slot_a], sems.at[1]),
        pltpu.make_async_copy(pay_ref.at[pl.ds(EDGES, 8)], halo.at[2], sems.at[2]),
        pltpu.make_async_copy(ra_ref.at[EDGES + 8], offs.at[slot_a], sems.at[3]),
        pltpu.make_async_copy(rb_ref.at[EDGES + 8], offs.at[1 - slot_a], sems.at[4]),
        pltpu.make_async_copy(pay_ref.at[EDGES + 8], offs.at[2], sems.at[5]),
        pltpu.make_async_copy(blend_ref, blend, sems.at[6]),
    ]
    late = doubled(spread_ref, spread, sems.at[pl.ds(7, 2)])
    last = doubled(back_ref, back, sems.at[pl.ds(9, 2)])
    own = [
        pltpu.make_async_copy(own_ref.at[n], field.at[n, pl.ds(8 * LINE, ROWS * LINE), :], sems.at[11 + n])
        for n in range(2)
    ]
    for copy in small + edges + late + own + last:
        copy.start()
    lane = place(PLANES, 256)
    local = lane % 48
    plane = lax.broadcasted_iota(jnp.int32, (PLANES, 256), 0)
    rise = (plane % 8).astype(jnp.float32) * 0.125
    q = (local % 16) // 4
    by_plane = jnp.where(q == plane // 8, 1.0 - rise, 0.0) + jnp.where(q == plane // 8 + 1, rise, 0.0)
    by_plane = jnp.where(jnp.logical_and(q < 3, lane < 144), by_plane, 0.0)
    coarse_row = ((local // 16) * 4 + local % 4 - 4).astype(jnp.float32)
    for copy in small:
        copy.wait()

    @pl.loop(0, HEIGHT // 8)
    def _(group):
        block = jnp.where(group == 0, 0, jnp.where(group == 5, 1, 2))
        start = jnp.where(group == 0, ROWS - 8, jnp.where(group == 5, 0, 8 * (group - 1)))
        for i in range(8):
            g = offs[block, 0, start + i] + (group - 1).astype(jnp.float32)
            f = i / 8.0
            line = jnp.where(coarse_row == g, 1.0 - f, 0.0) + jnp.where(coarse_row == g + 1.0, f, 0.0)
            row = pl.multiple_of(PLANES * (8 * group + i), 16)
            weights[pl.ds(row, PLANES), :] = (by_plane * line).astype(jnp.bfloat16)

    @pl.loop(0, 2)
    def _(m):
        stack = jnp.concatenate([halo[j, 4 + 2 * m + i] for j in (0, 2, 1) for i in range(2)], axis=0)
        pieces = jnp.concatenate(split3(stack), axis=0)
        parts = jnp.dot(pieces, blend[...], preferred_element_type=jnp.float32)
        along = (parts[0:48] + parts[48:96] + parts[96:144]) * (time_step / 24.0)
        table = jnp.concatenate(split3(along), axis=0)
        res[...] = jnp.dot(weights[:, 0:144], table, preferred_element_type=jnp.float32)

        @pl.loop(0, HEIGHT // 2)
        def _(i):
            for j in range(4):
                for t in range(TILES):
                    row = pl.multiple_of((i * 4 + j) * (8 * COEFS) + 8 * (5 * (5 + m) + t), 8)
                    cf[pl.ds(row, 8), :] = res[
                        pl.ds(pl.multiple_of(32 * i + 8 * j, 8), 8), 128 * t : 128 * t + 128
                    ]

    owner = place(16, 128) // 8
    for copy in edges + late:
        copy.wait()

    @pl.loop(0, 2)
    def _(n):
        @pl.loop(0, PLANES)
        def _(p):
            tiles = [raw[n, p, :, 128 * c : 128 * c + 128] for c in range(4)]
            for side in range(2):
                both = jnp.concatenate([halo[j, 2 * side + 1 - n] for j in range(2)], axis=0)
                tiles.append(jnp.where(owner == p, both, 0.0))
            spread_lhs(lhs, pl.multiple_of(256 * n + 16 * p, 16), tiles)

    res[0:512, :] = jnp.dot(lhs[...], spread[...], preferred_element_type=jnp.float32)

    @pl.loop(0, 2)
    def _(n):
        scale = jnp.where(n == 0, time_step / 4.0, 1.0)
        for j in range(2):
            for p in range(PLANES):
                for t in range(TILES):
                    row = pl.multiple_of(256 * n + 16 * p + 8 * j, 8)
                    tile = res[pl.ds(row, 8), 128 * t : 128 * t + 128] * scale
                    start = 40 * j * LINE + 40 * (p // 8) + 8 * t + p % 8
                    field[n, pl.ds(start, 8, stride=LINE), :] = tile

    for copy in own:
        copy.wait()

    def tile(ref, r, pg, t):
        return ref[pl.ds(pl.multiple_of(r * LINE + 40 * pg + 8 * t, 8), 8), :]

    def put(ref, r, pg, t, value):
        ref[pl.ds(pl.multiple_of(r * LINE + 40 * pg + 8 * t, 8), 8), :] = value

    def coef(r, pg, c, t):
        return pl.ds(pl.multiple_of((r * 2 + pg) * (8 * COEFS) + 8 * (5 * c + t), 8), 8)

    def rows(low, high):
        def wrap(body):
            @pl.loop(0, (high - low) // 4)
            def _(i):
                for j in range(4):
                    body(low + 4 * i + j)

        return wrap

    @rows(2, HEIGHT - 2)
    def _(r):
        for pg in range(2):
            k = [tile(kt, r, pg, t) for t in range(TILES)]
            nxt = k[1:] + [pltpu.roll(k[0], 127, 1)]
            prv = [pltpu.roll(k[4], 1, 1)] + k[:4]
            for t in range(TILES):
                ke, kw = k[t] + tile(kt, r + 1, pg, t), k[t] + tile(kt, r - 1, pg, t)
                kn, ks = k[t] + nxt[t], k[t] + prv[t]
                u8, v8 = 8.0 * cf[coef(r, pg, 5, t), :], 8.0 * cf[coef(r, pg, 6, t), :]
                cf[coef(r, pg, 0, t), :] = ke - u8
                cf[coef(r, pg, 1, t), :] = kw + u8
                cf[coef(r, pg, 2, t), :] = kn - v8
                cf[coef(r, pg, 3, t), :] = ks + v8
                cf[coef(r, pg, 4, t), :] = 1.0 - ((ke + kw) + (kn + ks))

    def step(y, r, pg):
        c = [tile(y, r, pg, t) for t in range(TILES)]
        first, second = pltpu.roll(c[0], 127, 1), pltpu.roll(c[1], 127, 1)
        last, before = pltpu.roll(c[4], 1, 1), pltpu.roll(c[3], 1, 1)
        ext = [before, last] + c + [first, second]
        new = []
        for t in range(TILES):
            total = cf[coef(r, pg, 0, t), :] * tile(y, r + 1, pg, t) + cf[coef(r, pg, 1, t), :] * tile(y, r - 1, pg, t)
            total += cf[coef(r, pg, 5, t), :] * (tile(y, r + 2, pg, t) - tile(y, r - 2, pg, t))
            along = cf[coef(r, pg, 2, t), :] * ext[t + 3] + cf[coef(r, pg, 3, t), :] * ext[t + 1]
            along += cf[coef(r, pg, 6, t), :] * (ext[t + 4] - ext[t])
            new.append(total + along + cf[coef(r, pg, 4, t), :] * c[t])
        return new, c

    @rows(2, HEIGHT - 2)
    def _(r):
        for pg in range(2):
            new, _ = step(state, r, pg)
            for t in range(TILES):
                put(y2, r, pg, t, new[t])

    @rows(4, HEIGHT - 4)
    def _(r):
        for pg in range(2):
            new, c = step(y2, r, pg)
            for t in range(TILES):
                put(y3, r, pg, t, tile(state, r, pg, t) + (new[t] - c[t]))

    @rows(6, HEIGHT - 6)
    def _(r):
        for pg in range(2):
            new, c = step(y3, r, pg)
            for t in range(TILES):
                put(y4, r, pg, t, tile(state, r, pg, t) + 2.0 * (new[t] - c[t]))

    third = 1.0 / 3.0

    @rows(0, ROWS)
    def _(q):
        r = q + 8
        for pg in range(2):
            new, _ = step(y4, r, pg)
            for t in range(TILES):
                total = (tile(y2, r, pg, t) - tile(state, r, pg, t)) + (2.0 * tile(y3, r, pg, t) + new[t])
                start = 168 * 8 * pg + 8 * (5 * (q // 8) + t) + q % 8
                final[pl.ds(start, 8, stride=168), :] = total * third

    @pl.loop(0, PLANES)
    def _(p):
        for g in range(2):
            rows = pl.ds(pl.multiple_of(32 * p + 16 * g, 16), 16)
            for t in range(TILES):
                both = [
                    final[pl.ds(pl.multiple_of(168 * p + 8 * (5 * (2 * g + i) + t), 8), 8), :] for i in range(2)
                ]
                high, low = split2(jnp.concatenate(both, axis=0))
                lhs[rows, 128 * t : 128 * t + 128] = high
                lhs[rows, WIDTH + 128 * t : WIDTH + 128 * t + 128] = low

    for copy in last:
        copy.wait()
    copies = []
    for half in range(2):
        rows = 8 * ROWS
        result[8 * half : 8 * half + 8] = jnp.dot(
            lhs[rows * half : rows * (half + 1), 0 : 2 * WIDTH], back[...], preferred_element_type=jnp.float32
        ).reshape(8, ROWS, COLS)
        copy = pltpu.make_async_copy(
            result.at[pl.ds(8 * half, 8)], out_ref.at[pl.ds(8 * half, 8)], out_sem.at[half]
        )
        copy.start()
        copies.append(copy)
    for copy in copies:
        copy.wait()


def advance(shape, own, ra, rb, pay, spread, back, blend):
    line = pltpu.VMEM((HEIGHT * LINE, 128), jnp.float32)
    return pl.pallas_call(
        main_kernel,
        out_shape=jax.ShapeDtypeStruct(shape, jnp.float32),
        in_specs=[ANY] * 7,
        out_specs=ANY,
        scratch_shapes=[
            pltpu.VMEM((2, PLANES, 16, COLS), jnp.float32),
            pltpu.VMEM((3, 8, 8, 128), jnp.float32),
            pltpu.SMEM((3, 8, 128), jnp.float32),
            pltpu.VMEM((HEIGHT * PLANES, 256), jnp.bfloat16),
            pltpu.VMEM((ROWS * PLANES, 1536), jnp.bfloat16),
            pltpu.VMEM((1536, WIDTH), jnp.bfloat16),
            pltpu.VMEM((2 * WIDTH, COLS), jnp.bfloat16),
            pltpu.VMEM((128, WIDTH), jnp.bfloat16),
            pltpu.VMEM((HEIGHT * PLANES, WIDTH), jnp.float32),
            pltpu.VMEM((2, HEIGHT * LINE, 128), jnp.float32),
            line, line, line,
            pltpu.VMEM((HEIGHT * 2 * COEFS * 8, 128), jnp.float32),
            pltpu.VMEM((PLANES * 168, 128), jnp.float32),
            pltpu.VMEM((PLANES, ROWS, COLS), jnp.float32),
            pltpu.SemaphoreType.DMA((2, 2, 4)),
            pltpu.SemaphoreType.DMA((13,)),
            pltpu.SemaphoreType.DMA((2,)),
        ],
        compiler_params=pltpu.CompilerParams(vmem_limit_bytes=LIMIT),
        name="advance",
    )(own, ra, rb, pay, spread, back, blend)


def angle_tables():
    unit = 2.0 * np.pi / 1024
    col = np.arange(16)[:, None, None] * 64 - 1 + np.arange(128)[None, None, :]
    near = (np.arange(64)[None, :, None] * col % 1024) * unit
    far = (np.arange(16)[:, None] * 64 * col[0, :, :] % 1024) * unit
    cas = np.concatenate([np.cos(near) + np.sin(near), np.cos(near) - np.sin(near)], axis=2)
    turn = np.concatenate([np.cos(far), np.sin(far)], axis=0)
    return cas.astype(np.float32), turn.astype(np.float32)


def per_device(scalar, diffusivity, vel_modes, offsets):
    n_cols, n_rows = lax.axis_size("cols"), lax.axis_size("rows")
    raw, a, b = first_step(scalar, diffusivity, vel_modes)
    modes = lax.all_to_all(raw, "cols", 0, 0, tiled=True)
    cas, turn = (jnp.asarray(table) for table in angle_tables())
    ca = lax.ppermute(a, "cols", pairing(n_cols, 0))
    cb = lax.ppermute(b, "cols", pairing(n_cols, 1))
    off = offsets.reshape(1, 32)
    pa, pb = payloads(scalar, diffusivity, modes, cas, turn, ca, cb, off)
    ra = lax.ppermute(pa, "rows", pairing(n_rows, 0))
    rb = lax.ppermute(pb, "rows", pairing(n_rows, 1))
    spread, back, blend = (jnp.asarray(table) for table in tables())
    ca, cb, _ = lax.optimization_barrier((ca, cb, pa))
    own = own_rows(scalar, diffusivity, ca, cb, spread)
    return advance(scalar.shape, own, ra, rb, pa, spread, back, blend)


def solution(mesh):
    return jax.shard_map(
        per_device,
        mesh=mesh,
        in_specs=(
            P(None, "rows", "cols"),
            P(None, "rows", "cols"),
            P(None, "rows", "cols"),
            P("rows"),
        ),
        out_specs=P(None, "rows", "cols"),
        check_vma=False,
    )
```

```python
import jax
import jax.numpy as jnp
import numpy as np
from jax import lax
from jax.experimental import pallas as pl
from jax.experimental.pallas import tpu as pltpu
from jax.sharding import PartitionSpec as P

time_step = 0.25
HIGHEST = lax.Precision.HIGHEST

PLANES, ROWS, COLS = 16, 32, 512
HEIGHT, TILES = 48, 5
WIDTH = 128 * TILES
LINE = 88
COEFS = 36
ANY = pl.BlockSpec(memory_space=pl.ANY)
HBM = pl.BlockSpec(memory_space=pltpu.HBM)
VMEM = pl.BlockSpec(memory_space=pltpu.VMEM)
EDGES = 2 * 4 * PLANES
PAYLOAD = EDGES + 4 + 4 + 1
LIMIT = 67043328
BLANK = 4


def tables():
    lane = np.arange(WIDTH)
    column = 5 * (lane % 128) + lane // 128 - 8
    column = np.where(column < COLS + 8, column, -100)
    source = np.concatenate([np.arange(COLS), np.arange(128) % 8 - 8, np.arange(128) % 8 + COLS])
    spread = (source[:, None] == column[None, :]).astype(jnp.bfloat16)
    back = np.ascontiguousarray(spread[:COLS].T)
    x = np.where(column == -100, -1000, column + 8)
    base, part = x // 8, (x % 8) / 8.0
    coarse = np.arange(128)[:, None]
    blend = (coarse == base) * (1.0 - part) + (coarse == base + 1) * part
    return spread, back, blend.astype(jnp.bfloat16)


def pairing(count, shift):
    return [(i, (i + 1) % count if (i + shift) % 2 == 0 else (i - 1) % count) for i in range(count)]


def place(rows=8, lanes=128, dim=1):
    return lax.broadcasted_iota(jnp.int32, (rows, lanes), dim)


def first_kernel(s_ref, k_ref, v_hbm, raw_ref, a_ref, b_ref, buf, v_ref, sem, v_sem):
    modes = pltpu.make_async_copy(v_hbm, v_ref, v_sem)
    modes.start()
    copies = []
    for n, ref in enumerate((s_ref, k_ref)):
        for side, ct in enumerate((0, 3)):
            copy = pltpu.make_async_copy(
                ref.at[:, :, pl.ds(ct * 128, 128)], buf.at[n, side], sem.at[n, side]
            )
            copy.start()
            copies.append(copy)
    modes.wait()
    halves = [
        jnp.concatenate([v_ref[3 * m + q] for q in range(3)] + [jnp.zeros((BLANK, 64), jnp.float32)], axis=0)
        for m in range(2)
    ]
    raw = jnp.concatenate(halves, axis=1)
    for s in range(16):
        raw_ref[s] = raw
    even = lax.rem(lax.axis_index("cols"), 2) == 0
    for copy in copies:
        copy.wait()
    lane = place()
    for group in range(4):
        for n in range(2):
            ends = []
            for side in range(2):
                total = jnp.zeros((8, 128), jnp.float32)
                for p in range(PLANES):
                    tile = buf[n, side, p, 8 * group : 8 * group + 8, :]
                    moved = pltpu.roll(tile, (8 * p - (0 if side == 0 else 120)) % 128, 1)
                    total = jnp.where(lane // 8 == p, moved, total)
                ends.append(total)
            a_ref[2 * group + n] = jnp.where(even, ends[1], ends[0])
            b_ref[2 * group + n] = jnp.where(even, ends[0], ends[1])


def first_step(scalar, diffusivity, vel_modes):
    return pl.pallas_call(
        first_kernel,
        out_shape=[jax.ShapeDtypeStruct((16, 16, 128), jnp.float32)]
        + [jax.ShapeDtypeStruct((8, 8, 128), jnp.float32)] * 2,
        in_specs=[HBM, HBM, HBM],
        out_specs=[VMEM] * 3,
        scratch_shapes=[
            pltpu.VMEM((2, 2, PLANES, ROWS, 128), jnp.float32),
            pltpu.VMEM((6, 4, 64), jnp.float32),
            pltpu.SemaphoreType.DMA((2, 2)),
            pltpu.SemaphoreType.DMA,
        ],
        compiler_params=pltpu.CompilerParams(vmem_limit_bytes=LIMIT),
        name="first",
    )(scalar, diffusivity, vel_modes)


def payload_kernel(
    s_ref, k_ref, modes_hbm, cas_ref, turn_hbm, ca_hbm, cb_hbm, off_hbm, pa_ref, pb_ref,
    stage, cas, modes_ref, turn_ref, ca_ref, cb_ref, off_ref, sem, cas_sem, out_sem,
):
    even = lax.rem(lax.axis_index("rows"), 2) == 0
    column = lax.axis_index("cols")
    fetch = [
        pltpu.make_async_copy(
            cas_ref.at[column], cas.at[pl.ds(64 * m, 64), pl.ds(256 * m, 256)], cas_sem.at[m]
        )
        for m in range(2)
    ]
    for i, (source, target) in enumerate(
        ((modes_hbm, modes_ref), (turn_hbm, turn_ref), (ca_hbm, ca_ref), (cb_hbm, cb_ref), (off_hbm, off_ref))
    ):
        fetch.append(pltpu.make_async_copy(source, target, cas_sem.at[2 + i]))
    for copy in fetch:
        copy.start()
    for m in range(2):
        cas[64 * m : 64 * m + 64, 256 * (1 - m) : 256 * (2 - m)] = jnp.zeros((64, 256), jnp.float32)
    col_even = lax.rem(lax.axis_index("cols"), 2) == 0
    group_a = jnp.where(even, 3, 0)
    copies = []
    for side, group in enumerate((group_a, 3 - group_a)):
        for n, ref in enumerate((s_ref, k_ref)):
            for ct in range(4):
                copy = pltpu.make_async_copy(
                    ref.at[:, pl.ds(pl.multiple_of(8 * group, 8), 8), pl.ds(ct * 128, 128)],
                    stage.at[side, pl.ds((4 * n + ct) * PLANES, PLANES)],
                    sem.at[n, ct, side],
                )
                copy.start()
                copies.append(copy)
    for copy in fetch:
        copy.wait()
    modes = modes_ref[...].reshape(16 * 16, 128)
    sent = []
    for side, out in enumerate((pa_ref, pb_ref)):
        for copy in copies[8 * side : 8 * side + 8]:
            copy.wait()
        copy = pltpu.make_async_copy(
            stage.at[side, pl.ds(0, EDGES)], out.at[pl.ds(0, EDGES)], out_sem.at[side, 0]
        )
        copy.start()
        sent.append(copy)
    partial = jnp.dot(modes, cas[...], precision=HIGHEST, preferred_element_type=jnp.float32)
    for m in range(2):
        physical = jnp.zeros((16, 128), jnp.float32)
        for s in range(16):
            part = partial[16 * s : 16 * s + 16, 256 * m : 256 * m + 256]
            physical += part[:, :128] * turn_ref[s : s + 1, :] + part[:, 128:] * turn_ref[16 + s : 17 + s, :]
        for side in range(2):
            for i in range(2):
                stage[side, EDGES + 4 + 2 * m + i] = physical[8 * i : 8 * i + 8]
    for side, (out, group) in enumerate(((pa_ref, group_a), (pb_ref, 3 - group_a))):
        for n in range(2):
            a, b = ca_ref[2 * group + n], cb_ref[2 * group + n]
            stage[side, EDGES + n] = jnp.where(col_even, b, a)
            stage[side, EDGES + 2 + n] = jnp.where(col_even, a, b)
        line = jnp.concatenate([off_ref[...].astype(jnp.float32), jnp.zeros((1, 96), jnp.float32)], axis=1)
        stage[side, EDGES + 8] = jnp.broadcast_to(line, (8, 128))
        copy = pltpu.make_async_copy(
            stage.at[side, pl.ds(EDGES, 9)], out.at[pl.ds(EDGES, 9)], out_sem.at[side, 1]
        )
        copy.start()
        sent.append(copy)
    for copy in sent:
        copy.wait()


def payloads(*args):
    return pl.pallas_call(
        payload_kernel,
        out_shape=[jax.ShapeDtypeStruct((PAYLOAD, 8, 128), jnp.float32)] * 2,
        in_specs=[HBM] * 8,
        out_specs=[HBM, HBM],
        scratch_shapes=[
            pltpu.VMEM((2, PAYLOAD, 8, 128), jnp.float32),
            pltpu.VMEM((128, 512), jnp.float32),
            pltpu.VMEM((16, 16, 128), jnp.float32),
            pltpu.VMEM((32, 128), jnp.float32),
            pltpu.VMEM((8, 8, 128), jnp.float32),
            pltpu.VMEM((8, 8, 128), jnp.float32),
            pltpu.VMEM((1, 32), jnp.int32),
            pltpu.SemaphoreType.DMA((2, 4, 2)),
            pltpu.SemaphoreType.DMA((7,)),
            pltpu.SemaphoreType.DMA((2, 2)),
        ],
        compiler_params=pltpu.CompilerParams(vmem_limit_bytes=LIMIT),
        name="payloads",
    )(*args)


def split2(value):
    high = value.astype(jnp.bfloat16)
    return high, (value - high.astype(jnp.float32)).astype(jnp.bfloat16)


def split3(value):
    high, _ = split2(value)
    middle, low = split2(value - high.astype(jnp.float32))
    return high, middle, low


def spread_lhs(lhs, row, tiles):
    for c, tile in enumerate(tiles):
        high, low = split2(tile)
        lhs[pl.ds(row, 16), 128 * c : 128 * c + 128] = high
        lhs[pl.ds(row, 16), 768 + 128 * c : 896 + 128 * c] = low


def doubled(ref, table, sem):
    rows = ref.shape[0]
    return [pltpu.make_async_copy(ref, table.at[pl.ds(half * rows, rows), :], sem.at[half]) for half in range(2)]


def own_kernel(
    s_ref, k_ref, ca_hbm, cb_hbm, spread_ref, out_ref,
    raw, cols, strip, lhs, spread, res, inner, sem, sems, out_sem,
):
    col_even = lax.rem(lax.axis_index("cols"), 2) == 0
    big = [pltpu.make_async_copy(ref, raw.at[n], sem.at[n]) for n, ref in enumerate((k_ref, s_ref))]
    late = doubled(spread_ref, spread, sems)
    small = [
        pltpu.make_async_copy(ref, cols.at[side], sems.at[2 + side]) for side, ref in enumerate((ca_hbm, cb_hbm))
    ]
    for copy in small + big[:1] + late + big[1:]:
        copy.start()
    for copy in small:
        copy.wait()
    for n in range(2):
        for group in range(4):
            a, b = cols[0, 2 * group + 1 - n], cols[1, 2 * group + 1 - n]
            strip[n, 0, 8 * group : 8 * group + 8, :] = jnp.where(col_even, b, a)
            strip[n, 1, 8 * group : 8 * group + 8, :] = jnp.where(col_even, a, b)
    owner = place(16, 128) // 8

    @pl.loop(0, 2)
    def _(n):
        pltpu.make_async_copy(k_ref, raw.at[n], sem.at[n]).wait()
        scale = jnp.where(n == 0, time_step / 4.0, 1.0)

        @pl.loop(0, PLANES)
        def _(p):
            for g in range(2):
                at = slice(16 * g, 16 * g + 16)
                tiles = [raw[n, p, at, 128 * c : 128 * c + 128] for c in range(4)]
                tiles += [jnp.where(owner == p, strip[n, side, at, :], 0.0) for side in range(2)]
                spread_lhs(lhs, pl.multiple_of(ROWS * p + 16 * g, 16), tiles)

        @pl.when(n == 0)
        def _():
            for copy in late:
                copy.wait()

        res[...] = jnp.dot(lhs[...], spread[...], preferred_element_type=jnp.float32)

        @pl.loop(0, ROWS // 8)
        def _(g):
            for p in range(PLANES):
                for t in range(TILES):
                    tile = res[pl.ds(pl.multiple_of(ROWS * p + 8 * g, 8), 8), 128 * t : 128 * t + 128] * scale
                    start = 8 * g * LINE + 40 * (p // 8) + 8 * t + p % 8
                    inner[n, pl.ds(start, 8, stride=LINE), :] = tile
            part = pl.ds(pl.multiple_of(8 * g * LINE, 8), 8 * LINE)
            pltpu.make_async_copy(inner.at[n, part], out_ref.at[n, part], out_sem.at[n]).start()

    for n in range(2):
        pltpu.make_async_copy(inner.at[n], out_ref.at[n], out_sem.at[n]).wait()


def own_rows(scalar, diffusivity, ca, cb, spread):
    return pl.pallas_call(
        own_kernel,
        out_shape=jax.ShapeDtypeStruct((2, ROWS * LINE, 128), jnp.float32),
        in_specs=[HBM] * 5,
        out_specs=HBM,
        scratch_shapes=[
            pltpu.VMEM((2, PLANES, ROWS, COLS), jnp.float32),
            pltpu.VMEM((2, 8, 8, 128), jnp.float32),
            pltpu.VMEM((2, 2, ROWS, 128), jnp.float32),
            pltpu.VMEM((ROWS * PLANES, 1536), jnp.bfloat16),
            pltpu.VMEM((1536, WIDTH), jnp.bfloat16),
            pltpu.VMEM((ROWS * PLANES, WIDTH), jnp.float32),
            pltpu.VMEM((2, ROWS * LINE, 128), jnp.float32),
            pltpu.SemaphoreType.DMA((2,)),
            pltpu.SemaphoreType.DMA((4,)),
            pltpu.SemaphoreType.DMA((2,)),
        ],
        compiler_params=pltpu.CompilerParams(vmem_limit_bytes=LIMIT),
        cost_estimate=pl.CostEstimate(flops=2_000_000_000, bytes_accessed=8_000_000, transcendentals=0),
        name="own_rows",
    )(scalar, diffusivity, ca, cb, spread)


def main_kernel(
    own_ref, ra_ref, rb_ref, pay_ref, spread_ref, back_ref, blend_ref, out_ref,
    raw, halo, offs, weights, lhs, spread, back, blend, res,
    field, y2, y3, y4, cf, final, result, sem, sems, out_sem,
):
    even = lax.rem(lax.axis_index("rows"), 2) == 0
    slot_a = jnp.where(even, 1, 0)
    kt, state = field.at[0], field.at[1]
    edges = []
    for side, (pay, slot) in enumerate(((ra_ref, slot_a), (rb_ref, 1 - slot_a))):
        for n in range(2):
            for ct in range(4):
                edges.append(
                    pltpu.make_async_copy(
                        pay.at[pl.ds((4 * (1 - n) + ct) * PLANES, PLANES)],
                        raw.at[n, :, pl.ds(pl.multiple_of(8 * slot, 8), 8), pl.ds(128 * ct, 128)],
                        sem.at[side, n, ct],
                    )
                )
    small = [
        pltpu.make_async_copy(ra_ref.at[pl.ds(EDGES, 8)], halo.at[slot_a], sems.at[0]),
        pltpu.make_async_copy(rb_ref.at[pl.ds(EDGES, 8)], halo.at[1 - slot_a], sems.at[1]),
        pltpu.make_async_copy(pay_ref.at[pl.ds(EDGES, 8)], halo.at[2], sems.at[2]),
        pltpu.make_async_copy(ra_ref.at[EDGES + 8], offs.at[slot_a], sems.at[3]),
        pltpu.make_async_copy(rb_ref.at[EDGES + 8], offs.at[1 - slot_a], sems.at[4]),
        pltpu.make_async_copy(pay_ref.at[EDGES + 8], offs.at[2], sems.at[5]),
        pltpu.make_async_copy(blend_ref, blend, sems.at[6]),
    ]
    late = doubled(spread_ref, spread, sems.at[pl.ds(7, 2)])
    last = doubled(back_ref, back, sems.at[pl.ds(9, 2)])
    own = [
        pltpu.make_async_copy(own_ref.at[n], field.at[n, pl.ds(8 * LINE, ROWS * LINE), :], sems.at[11 + n])
        for n in range(2)
    ]
    for copy in small + edges + late + own + last:
        copy.start()
    lane = place(PLANES, 256)
    local = lane % 48
    plane = lax.broadcasted_iota(jnp.int32, (PLANES, 256), 0)
    rise = (plane % 8).astype(jnp.float32) * 0.125
    q = (local % 16) // 4
    by_plane = jnp.where(q == plane // 8, 1.0 - rise, 0.0) + jnp.where(q == plane // 8 + 1, rise, 0.0)
    by_plane = jnp.where(jnp.logical_and(q < 3, lane < 144), by_plane, 0.0)
    coarse_row = ((local // 16) * 4 + local % 4 - 4).astype(jnp.float32)
    for copy in small:
        copy.wait()

    @pl.loop(0, HEIGHT // 8)
    def _(group):
        block = jnp.where(group == 0, 0, jnp.where(group == 5, 1, 2))
        start = jnp.where(group == 0, ROWS - 8, jnp.where(group == 5, 0, 8 * (group - 1)))
        for i in range(8):
            g = offs[block, 0, start + i] + (group - 1).astype(jnp.float32)
            f = i / 8.0
            line = jnp.where(coarse_row == g, 1.0 - f, 0.0) + jnp.where(coarse_row == g + 1.0, f, 0.0)
            row = pl.multiple_of(PLANES * (8 * group + i), 16)
            weights[pl.ds(row, PLANES), :] = (by_plane * line).astype(jnp.bfloat16)

    @pl.loop(0, 2)
    def _(m):
        stack = jnp.concatenate([halo[j, 4 + 2 * m + i] for j in (0, 2, 1) for i in range(2)], axis=0)
        pieces = jnp.concatenate(split3(stack), axis=0)
        parts = jnp.dot(pieces, blend[...], preferred_element_type=jnp.float32)
        along = (parts[0:48] + parts[48:96] + parts[96:144]) * (time_step / 24.0)
        table = jnp.concatenate(split3(along), axis=0)
        res[...] = jnp.dot(weights[:, 0:144], table, preferred_element_type=jnp.float32)

        @pl.loop(0, HEIGHT // 2)
        def _(i):
            for j in range(4):
                for t in range(TILES):
                    row = pl.multiple_of((i * 4 + j) * (8 * COEFS) + 8 * (5 * (5 + m) + t), 8)
                    cf[pl.ds(row, 8), :] = res[
                        pl.ds(pl.multiple_of(32 * i + 8 * j, 8), 8), 128 * t : 128 * t + 128
                    ]

    owner = place(16, 128) // 8
    for copy in edges + late:
        copy.wait()

    @pl.loop(0, 2)
    def _(n):
        @pl.loop(0, PLANES)
        def _(p):
            tiles = [raw[n, p, :, 128 * c : 128 * c + 128] for c in range(4)]
            for side in range(2):
                both = jnp.concatenate([halo[j, 2 * side + 1 - n] for j in range(2)], axis=0)
                tiles.append(jnp.where(owner == p, both, 0.0))
            spread_lhs(lhs, pl.multiple_of(256 * n + 16 * p, 16), tiles)

    res[0:512, :] = jnp.dot(lhs[...], spread[...], preferred_element_type=jnp.float32)

    @pl.loop(0, 2)
    def _(n):
        scale = jnp.where(n == 0, time_step / 4.0, 1.0)
        for j in range(2):
            for p in range(PLANES):
                for t in range(TILES):
                    row = pl.multiple_of(256 * n + 16 * p + 8 * j, 8)
                    tile = res[pl.ds(row, 8), 128 * t : 128 * t + 128] * scale
                    start = 40 * j * LINE + 40 * (p // 8) + 8 * t + p % 8
                    field[n, pl.ds(start, 8, stride=LINE), :] = tile

    for copy in own:
        copy.wait()

    def tile(ref, r, pg, t):
        return ref[pl.ds(pl.multiple_of(r * LINE + 40 * pg + 8 * t, 8), 8), :]

    def put(ref, r, pg, t, value):
        ref[pl.ds(pl.multiple_of(r * LINE + 40 * pg + 8 * t, 8), 8), :] = value

    def coef(r, pg, c, t):
        return pl.ds(pl.multiple_of((r * 2 + pg) * (8 * COEFS) + 8 * (5 * c + t), 8), 8)

    def rows(low, high):
        def wrap(body):
            @pl.loop(0, (high - low) // 4)
            def _(i):
                for j in range(4):
                    body(low + 4 * i + j)

        return wrap

    @rows(2, HEIGHT - 2)
    def _(r):
        for pg in range(2):
            k = [tile(kt, r, pg, t) for t in range(TILES)]
            nxt = k[1:] + [pltpu.roll(k[0], 127, 1)]
            prv = [pltpu.roll(k[4], 1, 1)] + k[:4]
            for t in range(TILES):
                ke, kw = k[t] + tile(kt, r + 1, pg, t), k[t] + tile(kt, r - 1, pg, t)
                kn, ks = k[t] + nxt[t], k[t] + prv[t]
                u8, v8 = 8.0 * cf[coef(r, pg, 5, t), :], 8.0 * cf[coef(r, pg, 6, t), :]
                cf[coef(r, pg, 0, t), :] = ke - u8
                cf[coef(r, pg, 1, t), :] = kw + u8
                cf[coef(r, pg, 2, t), :] = kn - v8
                cf[coef(r, pg, 3, t), :] = ks + v8
                cf[coef(r, pg, 4, t), :] = 1.0 - ((ke + kw) + (kn + ks))

    def step(y, r, pg):
        c = [tile(y, r, pg, t) for t in range(TILES)]
        first, second = pltpu.roll(c[0], 127, 1), pltpu.roll(c[1], 127, 1)
        last, before = pltpu.roll(c[4], 1, 1), pltpu.roll(c[3], 1, 1)
        ext = [before, last] + c + [first, second]
        new = []
        for t in range(TILES):
            total = cf[coef(r, pg, 0, t), :] * tile(y, r + 1, pg, t) + cf[coef(r, pg, 1, t), :] * tile(y, r - 1, pg, t)
            total += cf[coef(r, pg, 5, t), :] * (tile(y, r + 2, pg, t) - tile(y, r - 2, pg, t))
            along = cf[coef(r, pg, 2, t), :] * ext[t + 3] + cf[coef(r, pg, 3, t), :] * ext[t + 1]
            along += cf[coef(r, pg, 6, t), :] * (ext[t + 4] - ext[t])
            new.append(total + along + cf[coef(r, pg, 4, t), :] * c[t])
        return new, c

    @rows(2, HEIGHT - 2)
    def _(r):
        for pg in range(2):
            new, _ = step(state, r, pg)
            for t in range(TILES):
                put(y2, r, pg, t, new[t])

    @rows(4, HEIGHT - 4)
    def _(r):
        for pg in range(2):
            new, c = step(y2, r, pg)
            for t in range(TILES):
                put(y3, r, pg, t, tile(state, r, pg, t) + (new[t] - c[t]))

    @rows(6, HEIGHT - 6)
    def _(r):
        for pg in range(2):
            new, c = step(y3, r, pg)
            for t in range(TILES):
                put(y4, r, pg, t, tile(state, r, pg, t) + 2.0 * (new[t] - c[t]))

    third = 1.0 / 3.0

    @rows(0, ROWS)
    def _(q):
        r = q + 8
        for pg in range(2):
            new, _ = step(y4, r, pg)
            for t in range(TILES):
                total = (tile(y2, r, pg, t) - tile(state, r, pg, t)) + (2.0 * tile(y3, r, pg, t) + new[t])
                start = 168 * 8 * pg + 8 * (5 * (q // 8) + t) + q % 8
                final[pl.ds(start, 8, stride=168), :] = total * third

    @pl.loop(0, PLANES)
    def _(p):
        for g in range(2):
            rows = pl.ds(pl.multiple_of(32 * p + 16 * g, 16), 16)
            for t in range(TILES):
                both = [
                    final[pl.ds(pl.multiple_of(168 * p + 8 * (5 * (2 * g + i) + t), 8), 8), :] for i in range(2)
                ]
                high, low = split2(jnp.concatenate(both, axis=0))
                lhs[rows, 128 * t : 128 * t + 128] = high
                lhs[rows, WIDTH + 128 * t : WIDTH + 128 * t + 128] = low

    for copy in last:
        copy.wait()
    copies = []
    for half in range(2):
        rows = 8 * ROWS
        result[8 * half : 8 * half + 8] = jnp.dot(
            lhs[rows * half : rows * (half + 1), 0 : 2 * WIDTH], back[...], preferred_element_type=jnp.float32
        ).reshape(8, ROWS, COLS)
        copy = pltpu.make_async_copy(
            result.at[pl.ds(8 * half, 8)], out_ref.at[pl.ds(8 * half, 8)], out_sem.at[half]
        )
        copy.start()
        copies.append(copy)
    for copy in copies:
        copy.wait()


def advance(shape, own, ra, rb, pay, spread, back, blend):
    line = pltpu.VMEM((HEIGHT * LINE, 128), jnp.float32)
    return pl.pallas_call(
        main_kernel,
        out_shape=jax.ShapeDtypeStruct(shape, jnp.float32),
        in_specs=[ANY] * 7,
        out_specs=ANY,
        scratch_shapes=[
            pltpu.VMEM((2, PLANES, 16, COLS), jnp.float32),
            pltpu.VMEM((3, 8, 8, 128), jnp.float32),
            pltpu.SMEM((3, 8, 128), jnp.float32),
            pltpu.VMEM((HEIGHT * PLANES, 256), jnp.bfloat16),
            pltpu.VMEM((ROWS * PLANES, 1536), jnp.bfloat16),
            pltpu.VMEM((1536, WIDTH), jnp.bfloat16),
            pltpu.VMEM((2 * WIDTH, COLS), jnp.bfloat16),
            pltpu.VMEM((128, WIDTH), jnp.bfloat16),
            pltpu.VMEM((HEIGHT * PLANES, WIDTH), jnp.float32),
            pltpu.VMEM((2, HEIGHT * LINE, 128), jnp.float32),
            line, line, line,
            pltpu.VMEM((HEIGHT * 2 * COEFS * 8, 128), jnp.float32),
            pltpu.VMEM((PLANES * 168, 128), jnp.float32),
            pltpu.VMEM((PLANES, ROWS, COLS), jnp.float32),
            pltpu.SemaphoreType.DMA((2, 2, 4)),
            pltpu.SemaphoreType.DMA((13,)),
            pltpu.SemaphoreType.DMA((2,)),
        ],
        compiler_params=pltpu.CompilerParams(vmem_limit_bytes=LIMIT),
        name="advance",
    )(own, ra, rb, pay, spread, back, blend)


def angle_tables():
    unit = 2.0 * np.pi / 1024
    col = np.arange(16)[:, None, None] * 64 - 1 + np.arange(128)[None, None, :]
    near = (np.arange(64)[None, :, None] * col % 1024) * unit
    far = (np.arange(16)[:, None] * 64 * col[0, :, :] % 1024) * unit
    cas = np.concatenate([np.cos(near) + np.sin(near), np.cos(near) - np.sin(near)], axis=2)
    turn = np.concatenate([np.cos(far), np.sin(far)], axis=0)
    return cas.astype(np.float32), turn.astype(np.float32)


def per_device(scalar, diffusivity, vel_modes, offsets):
    n_cols, n_rows = lax.axis_size("cols"), lax.axis_size("rows")
    raw, a, b = first_step(scalar, diffusivity, vel_modes)
    modes = lax.all_to_all(raw, "cols", 0, 0, tiled=True)
    cas, turn = (jnp.asarray(table) for table in angle_tables())
    ca = lax.ppermute(a, "cols", pairing(n_cols, 0))
    cb = lax.ppermute(b, "cols", pairing(n_cols, 1))
    off = offsets.reshape(1, 32)
    pa, pb = payloads(scalar, diffusivity, modes, cas, turn, ca, cb, off)
    ra = lax.ppermute(pa, "rows", pairing(n_rows, 0))
    rb = lax.ppermute(pb, "rows", pairing(n_rows, 1))
    spread, back, blend = (jnp.asarray(table) for table in tables())
    ca, cb, _ = lax.optimization_barrier((ca, cb, pa))
    own = own_rows(scalar, diffusivity, ca, cb, spread)
    return advance(scalar.shape, own, ra, rb, pa, spread, back, blend)


def solution(mesh):
    return jax.shard_map(
        per_device,
        mesh=mesh,
        in_specs=(
            P(None, "rows", "cols"),
            P(None, "rows", "cols"),
            P(None, "rows", "cols"),
            P("rows"),
        ),
        out_specs=P(None, "rows", "cols"),
        check_vma=False,
    )
```
